32 devices in a mesh: gx: 8 (over y, x, core), gy: 4 (over z).
Axes of the slice: x: 2, y: 2, z: 4, core: 2. Of those that a mesh axis runs over, the one named last changes fastest.
Arguments:
- sky_interface_transfers: bfloat16 [4, 384, 1024], P(None, 'gy', 'gx'), may hold values from -6 to 6
- coupling_matrix_enlarged: bfloat16 [384, 1024, 128], P('gy', 'gx'), may hold values from -0.5 to 0.5
- piece_keeper_part: int32 [8, 384, 1], P('gx', 'gy'), may hold values from 0 to 31; in each aligned block of 96 rows (0 to 95, 96 to 191, ..., all dimensions but the last counted through in order) at most 6 rows name the same one
- receiving_part_line: int32 [8, 384], P('gx', 'gy'), may hold values from 0 to 127
- marine_point_switch: int32 [1024, 512], P('gx', 'gy'), may hold values 0 or 1
- potential_heat_deviation: float32 [8, 1024, 512], P(None, 'gx', 'gy'), may hold values from -6 to 6
- free_marine_lift: float32 [1024, 512], P('gx', 'gy'), may hold values from -3 to 3
- depth_averaged_uflow: float32 [1024, 512], P('gx', 'gy'), may hold values from -3 to 3
- depth_averaged_vflow: float32 [1024, 512], P('gx', 'gy'), may hold values from -3 to 3
Outputs:
- atmo_skin_temp_back: float32 [384, 1024], P('gy', 'gx')
- ocean_temp_after_step: float32 [8, 1024, 512], P(None, 'gx', 'gy')
- barotropic: float32 [3, 1024, 512], P(None, 'gx', 'gy')
The draws below stay inside these ranges and needn't reach their ends.
Inputs may be any that keep to these rules, and one draw needn't show every extreme that they name: `piece_keeper_part`: ocean devices are counted with gx slowest. Among the 96 blocks of one atmosphere device at most 6 have the same owner, and some device has exactly 6 with one owner; every ocean device owns some block.
All inputs are finite; a program needn't handle non-finite values. No bound on the sum of `marine_point_switch` on one device may be relied on, other than what follows from the above.
Results may differ from the reference program's by a relative error of at most 0.0026.
Values may be sent and summed in bfloat16 or wider, within the bound.
A program may use at most 64 MiB of HBM per device.

```python
import math
import jax
import jax.numpy as jnp
import numpy as np

NB = 96
BA = 128
OX = 128
BAND_NORTH_COUNT = 128
MARINE_STRATA = 8
SUB = 40
CAP = 6
ATMO_NS_TOTAL = 384
ATMO_EW_TOTAL = 1024
OCEANIC_EW_TOTAL = 1024
MARINE_LAT_SPAN = 512
N_GX = 8
N_GY = 4


def plant(values, stream_key, smallest, largest):
    place = [jax.random.randint(jax.random.fold_in(stream_key, axis), (), 0, length) for axis, length in enumerate(values.shape)]
    longest = values.shape.index(max(values.shape))
    next_to = place[:longest] + [(place[longest] + 1) % values.shape[longest]] + place[longest + 1:]
    return values.at[tuple(place)].set(smallest).at[tuple(next_to)].set(largest)


def block_levels(key, shape, split, least, top_value):
    def one(dim, parts):
        heights = jax.random.uniform(jax.random.fold_in(jax.random.fold_in(key, 6), dim), (parts,), jnp.float32, least / len(split), top_value / len(split))
        return jnp.repeat(jnp.exp(heights), shape[dim] // parts).reshape((-1,) + (1,) * (len(shape) - dim - 1))

    factor_of = one(*split[0])
    for cut in split[1:]:
        factor_of = factor_of * one(*cut)
    return factor_of


def assign_block(own_key, own, number, rows, count, top, limit, slope):
    sequence = jax.random.permutation(own_key, count)
    crowded, ordinary = portions_of(count, rows * top, limit, slope, True), portions_of(count, rows * top, limit, slope, False)
    places = jnp.arange(count)

    def named(sizes, turn):
        used = int((sizes > 0).sum())
        fixed = max(1, used // 4)
        passed = fixed + (places - fixed + turn * (used - fixed)) % max(1, count - fixed)
        return jnp.zeros((count,), jnp.int32).at[sequence[jnp.where(places < fixed, places, passed)]].set(jnp.asarray(sizes, jnp.int32))

    sizes = jnp.where(number % 4 == 0, named(crowded, number // 4), named(ordinary, number - number // 4 - 1))
    mixed = jax.random.permutation(jax.random.fold_in(own, 3), count)
    donor, taker = mixed[0:count // 2 * 2:2], mixed[1:count // 2 * 2:2]
    margin = jnp.minimum(sizes[donor] - 1, limit - sizes[taker]) // 2
    margin = jnp.where((donor == sequence[0]) | (taker == sequence[0]) | (sizes[taker] == 0), 0, jnp.maximum(margin, 0))
    passed = jax.random.randint(jax.random.fold_in(own, 4), (count // 2,), 0, 1 << 20) % (margin + 1)
    sizes = sizes.at[donor].add(-passed).at[taker].add(passed)
    items = jnp.searchsorted(jnp.cumsum(sizes), jnp.arange(rows * top), side="right").astype(jnp.int32)
    grid = items.reshape(top, rows).T
    grid = grid[jax.random.permutation(jax.random.fold_in(own, 1), rows)]
    turn = jax.random.randint(jax.random.fold_in(own, 2), (rows, 1), 0, top)
    return jnp.take_along_axis(grid, (jnp.arange(top)[None, :] + turn) % top, axis=1)


def portions_of(number_of, total, reach, slope, full):
    loads = [(1 << 20) // math.isqrt(rank ** slope) + 1 for rank in range(1, number_of + 1)]
    largest = reach if full else min(reach, max(-(-total // number_of), total * loads[0] // sum(loads)))
    least = 1 if total - largest >= number_of - 1 else 0
    counts, rest = [largest] + [least] * (number_of - 1), total - largest - least * (number_of - 1)
    while rest > 0:
        movable = [i for i in range(1, number_of) if counts[i] < largest] or [i for i in range(1, number_of) if counts[i] < reach]
        mass, budget = sum([loads[i] for i in movable]), rest
        for i in movable:
            addition = min(reach - counts[i], max(1, budget * loads[i] // mass), rest)
            counts[i] = counts[i] + addition
            rest = rest - addition
    return np.array(counts)


def bell_draw(stream_key, shape, scale, limit, split=(), kind=jnp.bfloat16):
    gain = block_levels(stream_key, shape, split, -0.22, 0.18) if split else 1.0
    entries = jax.random.normal(stream_key, shape, jnp.float32) * scale * gain
    return jnp.minimum(jnp.maximum(entries, -limit), limit).astype(kind)


def setup_inputs(seed: int = 0) -> dict:
    seeds = jax.random.split(jax.random.key(seed), 10)
    sky_interface_transfers = bell_draw(seeds[0], (4, ATMO_NS_TOTAL, ATMO_EW_TOTAL), 1.0, 6.0, ((1, 4), (2, 8)))
    coupling_matrix_enlarged = bell_draw(seeds[1], (ATMO_NS_TOTAL, ATMO_EW_TOTAL, BAND_NORTH_COUNT), BA ** -0.5, 0.5, ((0, 4), (1, 8)))
    piece_keeper_part_keys = jax.random.split(jax.random.fold_in(seeds[2], 1), N_GX * ATMO_NS_TOTAL // NB)
    piece_keeper_part_turns = jax.random.permutation(jax.random.fold_in(seeds[2], 3), N_GX * ATMO_NS_TOTAL // NB)
    piece_keeper_part = jax.vmap(lambda own, number: assign_block(jax.random.fold_in(seeds[2], 2), own, number, NB, N_GX * N_GY, 1, CAP, 2))(piece_keeper_part_keys, piece_keeper_part_turns).reshape((N_GX, ATMO_NS_TOTAL, 1))
    receiving_part_line = plant(jax.random.randint(seeds[3], (N_GX, ATMO_NS_TOTAL), 0, OX), jax.random.fold_in(seeds[3], 1), 0, OX - 1).astype(jnp.int32)
    marine_point_switch = plant((jax.random.randint(seeds[4], (OCEANIC_EW_TOTAL, MARINE_LAT_SPAN), 0, 8) < 7).astype(jnp.int32), jax.random.fold_in(seeds[4], 1), 0, 1)
    potential_heat_deviation = bell_draw(seeds[5], (MARINE_STRATA, OCEANIC_EW_TOTAL, MARINE_LAT_SPAN), 1.0, 6.0, ((1, 8), (2, 4)), jnp.float32)
    free_marine_lift = bell_draw(seeds[6], (OCEANIC_EW_TOTAL, MARINE_LAT_SPAN), 0.5, 3.0, ((0, 8), (1, 4)), jnp.float32)
    depth_averaged_uflow = bell_draw(seeds[7], (OCEANIC_EW_TOTAL, MARINE_LAT_SPAN), 0.5, 3.0, ((0, 8), (1, 4)), jnp.float32)
    depth_averaged_vflow = bell_draw(seeds[8], (OCEANIC_EW_TOTAL, MARINE_LAT_SPAN), 0.5, 3.0, ((0, 8), (1, 4)), jnp.float32)
    return {"sky_interface_transfers": sky_interface_transfers, "coupling_matrix_enlarged": coupling_matrix_enlarged, "piece_keeper_part": piece_keeper_part, "receiving_part_line": receiving_part_line, "marine_point_switch": marine_point_switch, "potential_heat_deviation": potential_heat_deviation, "free_marine_lift": free_marine_lift, "depth_averaged_uflow": depth_averaged_uflow, "depth_averaged_vflow": depth_averaged_vflow}


HORIZ_MIX = 0.15
VERT_MIX = 0.2
HEAT_GAIN = 0.5
FLOW_DAMP = 0.98
PRESS_GAIN = 0.6
DIVERGE_GAIN = 0.6
CORIOLIS = 0.1
WIND_GAIN = 0.05
FRESH_GAIN = 0.05


def velocity(height_rim, east_flow_component, north_flow_component, stress_east, stress_north, turning, liquid_portion):
    slope_east = height_rim[2:, 1:-1] - height_rim[:-2, 1:-1]
    slope_north = height_rim[1:-1, 2:] - height_rim[1:-1, :-2]
    zonal_new = (FLOW_DAMP * east_flow_component - PRESS_GAIN * slope_east + turning * north_flow_component + WIND_GAIN * stress_east) * liquid_portion
    merid_new = (FLOW_DAMP * north_flow_component - PRESS_GAIN * slope_north - turning * zonal_new + WIND_GAIN * stress_north) * liquid_portion
    return zonal_new, merid_new


def height(oceanic_top_sheet, zonal_rim, merid_rim, fresh_in, liquid_portion):
    spread = (zonal_rim[2:, 1:-1] - zonal_rim[:-2, 1:-1]) + (merid_rim[1:-1, 2:] - merid_rim[1:-1, :-2])
    return (oceanic_top_sheet - DIVERGE_GAIN * spread - FRESH_GAIN * fresh_in) * liquid_portion


def integrate_scalar_once(heat_deviation, heat_deviation_fringe, liquid_portion_fringe, incoming_enthalpy, liquid_portion):
    horizontal_diffusion = liquid_portion_fringe[2:, 1:-1] * (heat_deviation_fringe[:, 2:, 1:-1] - heat_deviation)
    horizontal_diffusion = horizontal_diffusion + liquid_portion_fringe[:-2, 1:-1] * (heat_deviation_fringe[:, :-2, 1:-1] - heat_deviation)
    horizontal_diffusion = horizontal_diffusion + liquid_portion_fringe[1:-1, 2:] * (heat_deviation_fringe[:, 1:-1, 2:] - heat_deviation)
    horizontal_diffusion = horizontal_diffusion + liquid_portion_fringe[1:-1, :-2] * (heat_deviation_fringe[:, 1:-1, :-2] - heat_deviation)
    above_level = jnp.concatenate([heat_deviation[:1], heat_deviation[:-1]], axis=0)
    below_level = jnp.concatenate([heat_deviation[1:], heat_deviation[-1:]], axis=0)
    vertical = (above_level - heat_deviation) + (below_level - heat_deviation)
    tendency = heat_deviation + HORIZ_MIX * horizontal_diffusion + VERT_MIX * vertical
    tendency = tendency.at[0].add(HEAT_GAIN * incoming_enthalpy)
    return tendency * liquid_portion


def reference(sky_interface_transfers, coupling_matrix_enlarged, piece_keeper_part, receiving_part_line, marine_point_switch, potential_heat_deviation, free_marine_lift, depth_averaged_uflow, depth_averaged_vflow):
    flux_blocks = sky_interface_transfers.astype(jnp.float32).reshape(4, ATMO_NS_TOTAL, N_GX, BA)
    subdomain_regrid_operator = coupling_matrix_enlarged.astype(jnp.float32).reshape(ATMO_NS_TOTAL, N_GX, BA, BAND_NORTH_COUNT)
    pieces = jnp.einsum("frgc,rgco->grfo", flux_blocks, subdomain_regrid_operator)
    target = piece_keeper_part[:, :, 0]
    flattened_sequence = (((target // N_GY) * OX + receiving_part_line) * N_GY + target % N_GY).astype(jnp.int32)
    collected = jnp.zeros((OCEANIC_EW_TOTAL * N_GY, 4, BAND_NORTH_COUNT), jnp.float32).at[flattened_sequence.reshape(-1)].add(pieces.reshape(-1, 4, BAND_NORTH_COUNT))
    marine_interface_transfers = collected.reshape(OCEANIC_EW_TOTAL, N_GY, 4, BAND_NORTH_COUNT).transpose(2, 0, 1, 3).reshape(4, OCEANIC_EW_TOTAL, MARINE_LAT_SPAN)
    rows_sea = jnp.arange(MARINE_LAT_SPAN, dtype=jnp.int32)
    wall_mask = ((rows_sea > 0) & (rows_sea < MARINE_LAT_SPAN - 1)).astype(jnp.float32)
    liquid_portion = marine_point_switch.astype(jnp.float32) * wall_mask[None, :]
    heat_deviation_fringe = jnp.pad(potential_heat_deviation, ((0, 0), (1, 1), (1, 1)), mode="wrap")
    liquid_portion_fringe = jnp.pad(liquid_portion, 1, mode="wrap")
    ocean_temp_after_step = integrate_scalar_once(potential_heat_deviation, heat_deviation_fringe, liquid_portion_fringe, marine_interface_transfers[2], liquid_portion)
    turning = CORIOLIS * jnp.sin(jnp.pi * ((rows_sea.astype(jnp.float32) + 0.5) / MARINE_LAT_SPAN - 0.5))[None, :]
    oceanic_top_sheet = free_marine_lift
    east_flow_component = depth_averaged_uflow
    north_flow_component = depth_averaged_vflow
    for substep in range(SUB):
        east_flow_component, north_flow_component = velocity(jnp.pad(oceanic_top_sheet, 1, mode="wrap"), east_flow_component, north_flow_component, marine_interface_transfers[0], marine_interface_transfers[1], turning, liquid_portion)
        flow_rim = jnp.pad(jnp.stack([east_flow_component, north_flow_component]), ((0, 0), (1, 1), (1, 1)), mode="wrap")
        oceanic_top_sheet = height(oceanic_top_sheet, flow_rim[0], flow_rim[1], marine_interface_transfers[3], liquid_portion)
    coupled_skin_warmness = ocean_temp_after_step[0].astype(jnp.bfloat16).reshape(OCEANIC_EW_TOTAL * N_GY, BAND_NORTH_COUNT)
    coupled_skin_warmness_band = coupled_skin_warmness[flattened_sequence]
    atmo_skin_temp_back = jnp.einsum("lpgm,plm->lpg", subdomain_regrid_operator, coupled_skin_warmness_band.astype(jnp.float32)).reshape(ATMO_NS_TOTAL, ATMO_EW_TOTAL)
    return atmo_skin_temp_back, ocean_temp_after_step, jnp.stack([oceanic_top_sheet, east_flow_component, north_flow_component])
```

```python
import jax
import jax.numpy as jnp
from jax import lax
from jax.experimental import pallas as pl
from jax.experimental.pallas import tpu as pltpu
from jax.sharding import PartitionSpec as P

NB = 96
OX = 128
BAND_NORTH_COUNT = 128
MARINE_STRATA = 8
SUB = 40


HORIZ_MIX = 0.15
VERT_MIX = 0.2
HEAT_GAIN = 0.5
FLOW_DAMP = 0.98
PRESS_GAIN = 0.6
DIVERGE_GAIN = 0.6
CORIOLIS = 0.1
WIND_GAIN = 0.05
FRESH_GAIN = 0.05


MESH = pl.DeviceIdType.MESH
LANES = BAND_NORTH_COUNT
HALF = LANES // 2
SPAN = SUB // 2
MARGIN = 2 * SPAN
BASE = MARGIN + 8
TALL = OX + 2 * BASE
FRAME = OX + 2 * MARGIN
OVERLAP = (LANES - 2 * MARGIN) // 2
GROUP = 4
RENEW = 3 * GROUP
CHUNK = 16
SLOTS = 8
FLUXES = 4
PARTS = 4


def turn_lanes(values, shift):
    shift = shift % LANES
    return pltpu.roll(values, shift, 1) if shift else values


def lanes(rows):
    return lax.broadcasted_iota(jnp.int32, (rows, LANES), 1)


def neighbours():
    nx, ny = lax.axis_size("gx"), lax.axis_size("gy")
    x, y = lax.axis_index("gx"), lax.axis_index("gy")
    up, down = lax.rem(x + 1, nx), lax.rem(x + nx - 1, nx)
    right, left = lax.rem(y + 1, ny), lax.rem(y + ny - 1, ny)
    return x, y, up, down, right, left


def peer_place(index):
    ny = lax.axis_size("gy")
    return lax.div(index, ny), lax.rem(index, ny)


def greet_all(me, count):
    barrier = pltpu.get_barrier_semaphore()

    def one(k, carry):
        place = peer_place(lax.rem(me + k, count))
        pl.semaphore_signal(barrier, inc=1, device_id=place, device_id_type=MESH)
        return carry

    lax.fori_loop(1, count, one, 0)


def peers(action, out, into, send_sem, recv_sem):
    nx, ny = lax.axis_size("gx"), lax.axis_size("gy")
    x, y = lax.axis_index("gx"), lax.axis_index("gy")
    me = x * ny + y
    for dy in sorted(range(ny), key=lambda d: abs(2 * d - ny)):

        def one(dx, carry, dy=dy):
            to_x, to_y = lax.rem(x + dx, nx), lax.rem(y + dy, ny)
            copy = pltpu.make_async_remote_copy(
                src_ref=out.at[to_x * ny + to_y],
                dst_ref=into.at[me],
                send_sem=send_sem.at[dx * ny + dy],
                recv_sem=recv_sem.at[dx * ny + dy],
                device_id=(to_x, to_y),
                device_id_type=MESH,
            )
            if action == "start":
                copy.start()
            else:
                copy.wait()
            return carry

        lax.fori_loop(0 if dy else 1, nx, one, 0)


def as_bits(condition):
    return jnp.where(condition, 1.0, 0.0).astype(jnp.bfloat16)


def line_numbers(shape, axis):
    return lax.broadcasted_iota(jnp.int32, shape, axis).astype(jnp.float32)


def dot(a, b, a_dim=1, b_dim=0):
    return lax.dot_general(
        a, b, (((a_dim,), (b_dim,)), ((), ())), preferred_element_type=jnp.float32
    )


def place_blocks(keeper, lines, count):
    i, j = line_numbers((NB, NB), 0), line_numbers((NB, NB), 1)
    owner_row = keeper[...].astype(jnp.float32)
    owner_col = jnp.sum(jnp.where(i == j, owner_row, 0.0), axis=1, keepdims=True)
    same = jnp.where(owner_col == owner_row, 1.0, 0.0)
    rank_row = jnp.sum(jnp.where(i < j, same, 0.0), axis=0, keepdims=True)
    rank_col = jnp.sum(jnp.where(j < i, same, 0.0), axis=1, keepdims=True)
    line_row = lines[...].astype(jnp.float32)
    line_col = jnp.sum(jnp.where(i == j, line_row, 0.0), axis=1, keepdims=True)
    owned = as_bits(line_numbers((count, NB), 0) == owner_row)
    ranked = jnp.where(line_numbers((NB, LANES), 1) == rank_col, line_col + 1.0, 0.0)
    listed = dot(owned, ranked.astype(jnp.bfloat16))
    return owner_row * SLOTS + rank_row, owner_col * SLOTS + rank_col, listed


def regrid(sky, weights, partial, waits):
    slot32 = lax.rem(lax.broadcasted_iota(jnp.int32, (FLUXES * SLOTS, LANES), 0), SLOTS)
    groups = NB // SLOTS
    for g in range(groups):
        if g % (groups // PARTS) == 0:
            waits[g // (groups // PARTS)].wait()
        rows = slice(g * SLOTS, (g + 1) * SLOTS)
        fluxes = sky[:, rows, :].astype(jnp.float32).reshape(FLUXES * SLOTS, OX)
        fluxes = fluxes.astype(jnp.bfloat16)
        total = dot(fluxes, weights[g * SLOTS])
        for n in range(1, SLOTS):
            total = jnp.where(slot32 == n, dot(fluxes, weights[g * SLOTS + n]), total)
        partial[:, rows, :] = total.reshape(FLUXES, SLOTS, LANES)


def fill_send(send, stage, partial, slots, count, most):
    rows = FLUXES * most
    pairs = []
    for f in range(0, FLUXES, 2):
        both = jnp.concatenate([partial[f], partial[f + 1]], axis=1).astype(jnp.bfloat16)
        pairs.append(dot(slots, both))
    for d in range(count):
        for f in range(FLUXES):
            at = d * rows + f * most
            from_lane = (f % 2) * LANES
            stage[at : at + SLOTS] = pairs[f // 2][
                d * SLOTS : (d + 1) * SLOTS, from_lane : from_lane + LANES
            ]
    send[...] = stage[0 : count * rows].reshape(count, rows, LANES).astype(jnp.bfloat16)


def read_targets(listed_in, count):
    lane = line_numbers((SLOTS, LANES), 1)
    row = line_numbers((SLOTS, LANES), 0)
    tiles = []
    for s in range(count):
        line = jnp.broadcast_to(listed_in[s], (SLOTS, LANES))
        line = jnp.sum(jnp.where(lane == row, line, 0.0), axis=1, keepdims=True)
        tiles.append(jnp.where(lane + 1.0 == line, 1.0, 0.0))
    return jnp.concatenate(tiles, axis=0)


def read_fluxes(recv, stage, count, most):
    rows = FLUXES * most
    stage[0 : count * rows] = recv[...].astype(jnp.float32).reshape(count * rows, LANES)
    values = []
    for f in range(FLUXES):
        starts = [s * rows + f * most for s in range(count)]
        tiles = [stage[at : at + SLOTS] for at in starts]
        values.append(jnp.concatenate(tiles, axis=0).astype(jnp.bfloat16))
    return values


def edge_selector(rows, low_row, high_row):
    row = lax.broadcasted_iota(jnp.int32, (rows, BAND_NORTH_COUNT), 0)
    lane = lax.broadcasted_iota(jnp.int32, (rows, BAND_NORTH_COUNT), 1)
    return as_bits(
        ((row == low_row) & (lane == 0)) | ((row == high_row) & (lane == BAND_NORTH_COUNT - 1))
    )


def fill_heat_edges(heat, edges):
    selector = edge_selector(8, 0, 1)
    for k in range(MARINE_STRATA):
        level = slice(k, k + 1)
        edges[0, level] = heat[k, 0:1]
        edges[1, level] = heat[k, OX - 1 : OX]
        sides = dot(selector, heat[k].astype(jnp.bfloat16), 1, 1)
        edges[2, level] = sides[0:1]
        edges[3, level] = sides[1:2]


def heat_copies(edges, got, send_sem, recv_sem):
    x, y, up, down, right, left = neighbours()
    plan = ((1, 0, (up, y)), (0, 1, (down, y)), (3, 2, (x, right)), (2, 3, (x, left)))
    return [
        pltpu.make_async_remote_copy(
            src_ref=edges.at[src],
            dst_ref=got.at[dst],
            send_sem=send_sem.at[k],
            recv_sem=recv_sem.at[k],
            device_id=place,
            device_id_type=MESH,
        )
        for k, (src, dst, place) in enumerate(plan)
    ]


def heat_step(heat, got, tall, shore, left_wet, right_wet, near, out):
    last = lanes(OX) == LANES - 1
    first = lanes(OX) == 0
    mine = shore[8 : 8 + OX]
    near[0] = jnp.where(last, turn_lanes(right_wet, -1), turn_lanes(mine, -1))
    near[1] = jnp.where(first, turn_lanes(left_wet, 1), turn_lanes(mine, 1))
    sides = jnp.concatenate([got[3], got[2]], axis=0).astype(jnp.bfloat16)
    for k in range(MARINE_STRATA):
        tall[k, 8 : 8 + OX] = heat[k]
        tall[k, 7:8] = got[0, k : k + 1]
        tall[k, 8 + OX : 9 + OX] = got[1, k : k + 1]
        near[2 + k] = dot(sides, edge_selector(2 * MARINE_STRATA, MARINE_STRATA + k, k), 0, 0)

    step = 32
    last, first = last[:step], first[:step]

    def one(k, carry):
        above, below = jnp.maximum(k - 1, 0), jnp.minimum(k + 1, MARINE_STRATA - 1)
        for start in range(0, OX, step):
            rows = slice(start, start + step)
            tall_rows = lambda shift: slice(8 + start + shift, 8 + start + step + shift)
            here = heat[k, rows]
            side = near[2 + k, rows]
            north = jnp.where(last, side, turn_lanes(here, -1))
            south = jnp.where(first, side, turn_lanes(here, 1))
            lateral = shore[tall_rows(1)] * (tall[k, tall_rows(1)] - here)
            lateral = lateral + shore[tall_rows(-1)] * (tall[k, tall_rows(-1)] - here)
            lateral = lateral + near[0, rows] * (north - here)
            lateral = lateral + near[1, rows] * (south - here)
            vertical = (heat[above, rows] - here) + (heat[below, rows] - here)
            out[k, rows] = (here + HORIZ_MIX * lateral + VERT_MIX * vertical) * shore[tall_rows(0)]
        return carry

    lax.fori_loop(0, MARINE_STRATA, one, 0)


def remote(src, dst, place, send, recv, k):
    return pltpu.make_async_remote_copy(
        src_ref=src,
        dst_ref=dst,
        send_sem=send.at[k],
        recv_sem=recv.at[k],
        device_id=place,
        device_id_type=MESH,
    )


class Exchange:
    def __init__(self, rows, edge, packs, sides, send, recv, wrap):
        x, y, up, down, right, left = neighbours()
        ny = lax.axis_size("gy")
        low, high = packs.at[0], packs.at[1]
        from_left, from_right = sides.at[0], sides.at[1]
        top, whole, bottom = pl.ds(OX - MARGIN, MARGIN), pl.ds(0, OX), pl.ds(0, MARGIN)
        before, middle, after = pl.ds(0, MARGIN), pl.ds(MARGIN, OX), pl.ds(MARGIN + OX, MARGIN)
        moves = ((top, before, up), (bottom, after, down), (whole, middle, x))
        self.rows = []
        if rows is not None:
            self.rows = [
                remote(rows.at[1], edge.at[0], (up, y), send, recv, 6),
                remote(rows.at[0], edge.at[1], (down, y), send, recv, 7),
            ]
        self.right = [
            remote(high.at[src], from_left.at[dst], (to, right), send, recv, k)
            for k, (src, dst, to) in enumerate(moves)
        ]
        self.left = [
            remote(low.at[src], from_right.at[dst], (to, left), send, recv, 3 + k)
            for k, (src, dst, to) in enumerate(moves)
        ]
        self.wrap, self.has_right, self.has_left = wrap, y < ny - 1, y > 0

    def guarded(self, condition, copies, action):
        def act():
            for copy in copies:
                getattr(copy, action)()

        if self.wrap:
            act()
        else:
            pl.when(condition)(act)

    def start(self):
        self.guarded(self.has_right, self.right, "start")
        self.guarded(self.has_left, self.left, "start")
        for copy in self.rows:
            copy.start()

    def wait(self):
        for copy in self.rows:
            copy.wait()
        self.guarded(self.has_left, self.right, "wait_recv")
        self.guarded(self.has_right, self.left, "wait_recv")
        self.guarded(self.has_right, self.right, "wait_send")
        self.guarded(self.has_left, self.left, "wait_send")


def clear_walls(sides):
    y, ny = lax.axis_index("gy"), lax.axis_size("gy")
    blank = jnp.zeros((FRAME, LANES), jnp.bfloat16)

    @pl.when(y == 0)
    def _():
        for side in sides:
            side[0] = blank

    @pl.when(y == ny - 1)
    def _():
        for side in sides:
            side[1] = blank


def fill_rows(rows, field, values):
    rows[0, field] = values[:MARGIN].astype(jnp.bfloat16)
    rows[1, field] = values[OX - MARGIN :].astype(jnp.bfloat16)


def fill_packs(packs, values):
    lane = lanes(OX)
    low = turn_lanes(values[2], LANES - 3 * MARGIN)
    low = jnp.where(lane >= LANES - 2 * MARGIN, turn_lanes(values[1], LANES - 2 * MARGIN), low)
    low = jnp.where(lane >= LANES - MARGIN, turn_lanes(values[0], LANES - MARGIN), low)
    high = turn_lanes(values[2], 3 * MARGIN)
    high = jnp.where(lane < 2 * MARGIN, turn_lanes(values[1], 2 * MARGIN), high)
    high = jnp.where(lane < MARGIN, turn_lanes(values[0], MARGIN), high)
    packs[0] = low.astype(jnp.bfloat16)
    packs[1] = high.astype(jnp.bfloat16)


def zones():
    return (
        (BASE - MARGIN, 0, MARGIN, 0),
        (BASE, MARGIN, OX, None),
        (BASE + OX, MARGIN + OX, MARGIN, 1),
    )


def spread_fields(natural, edge, sides, wide, mask):
    for at, side_at, size, end in zones():
        lane = lanes(size)
        here, there = slice(at, at + size), slice(side_at, side_at + size)
        from_left = sides[0, there].astype(jnp.float32)
        from_right = sides[1, there].astype(jnp.float32)
        for f in range(3):
            centre = natural[f] if end is None else edge[end, f].astype(jnp.float32)
            left = turn_lanes(from_left, -f * MARGIN)
            right = turn_lanes(from_right, f * MARGIN)
            one = jnp.where(lane < MARGIN, left, turn_lanes(centre, MARGIN))
            two = jnp.where(lane >= LANES - MARGIN, right, turn_lanes(centre, -MARGIN))
            if mask is not None and f > 0:
                one = jnp.where(mask[0, here] > 0, one, 0.0)
                two = jnp.where(mask[1, here] > 0, two, 0.0)
            wide[f, 0, here] = one
            wide[f, 1, here] = two


def spread_wet(shore, edge, sides, gain):
    for at, side_at, size, end in zones():
        lane = lanes(size)
        here, there = slice(at, at + size), slice(side_at, side_at + size)
        from_left = sides[0, there].astype(jnp.float32)
        from_right = sides[1, there].astype(jnp.float32)
        centre = shore[8 : 8 + OX] if end is None else edge[end, 3].astype(jnp.float32)
        one = jnp.where(lane >= LANES - MARGIN, from_left, centre)
        two = jnp.where(lane < MARGIN, from_right, centre)
        gain[0, here] = PRESS_GAIN * turn_lanes(one, MARGIN)
        gain[1, here] = PRESS_GAIN * turn_lanes(two, -MARGIN)


def renew_overlap(state, reach):
    low, high = BASE - reach, BASE + OX + reach
    shift = LANES - 2 * MARGIN + 2 * OVERLAP
    for start in range(low, high, CHUNK):
        rows = slice(start, start + CHUNK)
        lane = lanes(CHUNK)
        for f in range(3):
            one, two = state[f, 0, rows], state[f, 1, rows]
            state[f, 0, rows] = jnp.where(lane >= LANES - OVERLAP, turn_lanes(two, 2 * MARGIN), one)
            state[f, 1, rows] = jnp.where(lane < OVERLAP, turn_lanes(one, -2 * MARGIN), two)


def own_part(state, f, rows=None):
    one, two = state[f, 0, BASE : BASE + OX], state[f, 1, BASE : BASE + OX]
    return jnp.where(lanes(OX) < HALF, turn_lanes(one, -MARGIN), turn_lanes(two, MARGIN))


def substep(reach, state, forces, gain, turning, raw):
    low, high = BASE - reach, BASE + OX + reach
    turn = [jnp.broadcast_to(turning[tile : tile + 1, :], (CHUNK, LANES)) for tile in range(2)]

    def velocity(start, tile):
        rows = slice(start, start + CHUNK)
        height = state[0, tile, rows]
        slope_east = (
            state[0, tile, start + 1 : start + CHUNK + 1]
            - state[0, tile, start - 1 : start + CHUNK - 1]
        )
        slope_north = turn_lanes(height, -1) - turn_lanes(height, 1)
        old_u, old_v, slope = state[1, tile, rows], state[2, tile, rows], gain[tile, rows]
        new_u = (FLOW_DAMP * old_u + turn[tile] * old_v) + (
            forces[0, tile, rows] - slope * slope_east
        )
        new_v = (FLOW_DAMP * old_v + (forces[1, tile, rows] - slope * slope_north)) - (
            turn[tile] * new_u
        )
        state[1, tile, rows] = new_u
        state[2, tile, rows] = new_v

    def surface(start, tile):
        rows = slice(start, start + CHUNK)
        flow_north = state[2, tile, rows]
        spread_east = (
            state[1, tile, start + 1 : start + CHUNK + 1]
            - state[1, tile, start - 1 : start + CHUNK - 1]
        )
        spread_north = turn_lanes(flow_north, -1) - turn_lanes(flow_north, 1)
        height, slope = state[0, tile, rows], gain[tile, rows]
        if raw:
            height = jnp.where(slope > 0, height, 0.0)
        state[0, tile, rows] = (height - forces[2, tile, rows]) - slope * (
            spread_east + spread_north
        )

    starts = range(low, high, CHUNK)
    for start in starts:
        for tile in range(2):
            velocity(start, tile)
        if start > low:
            for tile in range(2):
                surface(start - CHUNK, tile)
    for tile in range(2):
        surface(high - CHUNK, tile)


def run_span(state, forces, gain, turning, raw):
    done = 0
    while done < SPAN:
        need = 2 * (SPAN - done) - 1
        reach = -(-need // 8) * 8
        steps = min(SPAN - done, GROUP)
        if done == RENEW:
            renew_overlap(state, reach)
        if raw and done == 0:
            substep(reach, state, forces, gain, turning, True)

        def one(_, carry, reach=reach):
            substep(reach, state, forces, gain, turning, False)
            return carry

        lax.fori_loop(1 if raw and done == 0 else 0, steps, one, 0)
        done += steps


def window_kernel(
    sky_far, weights_far, keeper_far, lines_far, sea_far, heat_far, h_far, u_far, v_far,
    back, heat_out, out,
    sky, weights, keeper, lines, sea, heat, natural,
    turning, partial, stage, send, recv, listed_out, listed_in, skin_send, skin_recv,
    heat_edges, heat_got, tall, near, shore,
    state, forces, gain,
    rows1, edge1, packs1, sides1, wets, wets_in,
    rows2, edge2, packs2, sides2, rows3, edge3, packs3, sides3,
    load_sem, list_send, list_recv, a2a_send, a2a_recv, skin_send_sem, skin_recv_sem,
    heat_send_sem, heat_recv_sem, send0, recv0, send1, recv1, send2, recv2, send3, recv3,
):
    ny = lax.axis_size("gy")
    count = lax.axis_size("gx") * ny
    most = max(2, 2 * NB // count)
    me = lax.axis_index("gx") * ny + lax.axis_index("gy")
    greet_all(me, count)
    part = NB // PARTS
    pieces = [pl.ds(p * part, part) for p in range(PARTS)]
    moves = [(keeper_far, keeper), (lines_far, lines), (sky_far, sky)]
    moves += [(weights_far.at[piece], weights.at[piece]) for piece in pieces]
    moves += [(sea_far, sea), (h_far, natural.at[0]), (u_far, natural.at[1])]
    moves += [(v_far, natural.at[2]), (heat_far, heat)]
    loads = [
        pltpu.make_async_copy(src, dst, load_sem.at[k]) for k, (src, dst) in enumerate(moves)
    ]
    for load in loads:
        load.start()
    turning[...] = turning_rows()
    clear_walls((sides2, sides3, wets_in))
    blank = jnp.zeros((8, LANES), jnp.float32)
    for f in range(2):
        for tile in range(2):
            state[f, tile, BASE - MARGIN - 8 : BASE - MARGIN] = blank
            state[f, tile, BASE + OX + MARGIN : BASE + OX + MARGIN + 8] = blank
    stage[count * FLUXES * most : count * FLUXES * most + SLOTS] = blank
    loads[0].wait()
    loads[1].wait()
    key_row, key_col, listed = place_blocks(keeper, lines, count)
    for d in range(count):
        listed_out[d] = listed[d : d + 1]
    slots = as_bits(line_numbers((count * SLOTS, NB), 0) == key_row)
    loads[2].wait()
    regrid(sky, weights, partial, loads[3 : 3 + PARTS])
    fill_send(send, stage, partial, slots, count, most)
    pl.semaphore_wait(pltpu.get_barrier_semaphore(), count - 1)
    peers("start", listed_out, listed_in, list_send, list_recv)
    peers("start", send, recv, a2a_send, a2a_recv)
    recv[me] = send[me]
    listed_in[me] = listed_out[me]
    for load in loads[3 + PARTS :]:
        load.wait()
    lat = lax.axis_index("gy") * LANES + lanes(OX)
    inside = (lat > 0) & (lat < ny * LANES - 1)
    shore[8 : 8 + OX] = jnp.where(inside, sea[...].astype(jnp.float32), 0.0)
    fill_heat_edges(heat, heat_edges)
    heats = heat_copies(heat_edges, heat_got, heat_send_sem, heat_recv_sem)
    for copy in heats:
        copy.start()
    for f in range(3):
        fill_rows(rows1, f, natural[f])
    fill_rows(rows1, 3, shore[8 : 8 + OX])
    fill_packs(packs1, [natural[f] for f in range(3)])
    wets[0] = shore[8 : 8 + OX].astype(jnp.bfloat16)
    wets[1] = shore[8 : 8 + OX].astype(jnp.bfloat16)
    first = Exchange(rows1, edge1, packs1, sides1, send1, recv1, True)
    wet = Exchange(None, None, wets, wets_in, send0, recv0, False)
    wet.start()
    first.start()
    peers("wait", listed_out, listed_in, list_send, list_recv)
    target = read_targets(listed_in, count)
    target_turned = target.T.astype(jnp.bfloat16)
    target = target.astype(jnp.bfloat16)
    peers("wait", send, recv, a2a_send, a2a_recv)
    values = read_fluxes(recv, stage, count, most)
    stress = dot(target_turned, jnp.concatenate([values[0], values[1]], axis=1))
    others = dot(target_turned, jnp.concatenate([values[3], values[2]], axis=1))
    mask = shore[8 : 8 + OX]
    own = [
        WIND_GAIN * stress[:, :LANES] * mask,
        WIND_GAIN * stress[:, LANES:] * mask,
        FRESH_GAIN * others[:, :LANES] * mask,
    ]
    for f in range(3):
        fill_rows(rows2, f, own[f])
    fill_packs(packs2, own)
    second = Exchange(rows2, edge2, packs2, sides2, send2, recv2, False)
    second.start()
    wet.wait()
    first.wait()
    for copy in heats:
        copy.wait()
    spread_wet(shore, edge1, wets_in, gain)
    spread_fields(natural, edge1, sides1, state, gain)
    shore[7:8] = edge1[0, 3, MARGIN - 8 : MARGIN].astype(jnp.float32)[7:8]
    shore[8 + OX : 9 + OX] = edge1[1, 3, 0:8].astype(jnp.float32)[0:1]
    left_wet = wets_in[0, MARGIN : MARGIN + OX].astype(jnp.float32)
    right_wet = wets_in[1, MARGIN : MARGIN + OX].astype(jnp.float32)
    heat_step(heat, heat_got, tall, shore, left_wet, right_wet, near, heat_out)
    surface = heat_out[0] + HEAT_GAIN * others[:, LANES:] * shore[8 : 8 + OX]
    heat_out[0] = surface
    band = dot(target, surface.astype(jnp.bfloat16))
    skin_send[...] = band.reshape(count, SLOTS, LANES).astype(jnp.bfloat16)
    peers("start", skin_send, skin_recv, skin_send_sem, skin_recv_sem)
    skin_recv[me] = skin_send[me]
    second.wait()
    spread_fields(own, edge2, sides2, forces, None)
    run_span(state, forces, gain, turning, True)
    for f in range(3):
        natural[f] = own_part(state, f)
        fill_rows(rows3, f, natural[f])
    fill_packs(packs3, [natural[f] for f in range(3)])
    third = Exchange(rows3, edge3, packs3, sides3, send3, recv3, False)
    third.start()
    peers("wait", skin_send, skin_recv, skin_send_sem, skin_recv_sem)
    slots = as_bits(line_numbers((NB, count * SLOTS), 1) == key_col)
    skin = dot(slots, skin_recv[...].reshape(count * SLOTS, LANES))
    slot8 = lax.broadcasted_iota(jnp.int32, (SLOTS, LANES), 0)
    for g in range(NB // SLOTS):
        rows = slice(g * SLOTS, (g + 1) * SLOTS)
        lines_skin = skin[rows].astype(jnp.bfloat16)
        total = dot(lines_skin, weights[g * SLOTS], 1, 1)
        for n in range(1, SLOTS):
            total = jnp.where(slot8 == n, dot(lines_skin, weights[g * SLOTS + n], 1, 1), total)
        back[rows] = total
    third.wait()
    spread_fields(natural, edge3, sides3, state, None)
    run_span(state, forces, gain, turning, False)
    for f in range(3):
        out[f] = own_part(state, f)


def turning_rows():
    total_y = lax.axis_size("gy") * LANES
    shape = (8, LANES)
    lane = lax.broadcasted_iota(jnp.int32, shape, 1)
    tile = lax.broadcasted_iota(jnp.int32, shape, 0)
    rows = lax.axis_index("gy") * LANES + lane + jnp.where(tile == 0, -MARGIN, MARGIN)
    rows = jnp.where(rows < 0, rows + total_y, jnp.where(rows < total_y, rows, rows - total_y))
    return CORIOLIS * jnp.sin(jnp.pi * ((rows.astype(jnp.float32) + 0.5) / total_y - 0.5))


def hand_over(*refs):
    sources, targets = refs[:3], refs[3:6]
    buffers, loads, stores = refs[6:9], refs[9], refs[10]
    into = [
        pltpu.make_async_copy(sources[k], buffers[k], loads.at[k]) for k in range(3)
    ]
    away = [
        pltpu.make_async_copy(buffers[k], targets[k], stores.at[k]) for k in range(3)
    ]
    for copy in into:
        copy.start()
    for k in range(3):
        into[k].wait()
        away[k].start()
    for copy in away:
        copy.wait()


def per_device(
    sky_interface_transfers,
    coupling_matrix_enlarged,
    piece_keeper_part,
    receiving_part_line,
    marine_point_switch,
    potential_heat_deviation,
    free_marine_lift,
    depth_averaged_uflow,
    depth_averaged_vflow,
):
    count = lax.axis_size("gx") * lax.axis_size("gy")
    most = max(2, 2 * NB // count)
    line = LANES
    half = jnp.bfloat16
    full = jnp.float32

    def boxes(fields):
        return [
            pltpu.VMEM((2, fields, MARGIN, line), half),
            pltpu.VMEM((2, fields, MARGIN, line), half),
            pltpu.VMEM((2, OX, line), half),
            pltpu.VMEM((2, FRAME, line), half),
        ]

    inside = pl.BlockSpec(memory_space=pltpu.VMEM)
    far = pl.BlockSpec(memory_space=pltpu.HBM)
    shapes = (
        jax.ShapeDtypeStruct((NB, OX), full),
        jax.ShapeDtypeStruct((MARINE_STRATA, OX, line), full),
        jax.ShapeDtypeStruct((3, OX, line), full),
    )
    results = pl.pallas_call(
        window_kernel,
        out_shape=shapes,
        in_specs=[far] * 9,
        out_specs=(inside,) * 3,
        scratch_shapes=[
            pltpu.VMEM((FLUXES, NB, OX), half),
            pltpu.VMEM((NB, OX, line), half),
            pltpu.VMEM((1, NB), jnp.int32),
            pltpu.VMEM((1, NB), jnp.int32),
            pltpu.VMEM((OX, line), jnp.int32),
            pltpu.VMEM((MARINE_STRATA, OX, line), full),
            pltpu.VMEM((3, OX, line), full),
            pltpu.VMEM((8, line), full),
            pltpu.VMEM((FLUXES, NB, line), full),
            pltpu.VMEM((count * FLUXES * most + SLOTS, line), full),
            pltpu.VMEM((count, FLUXES * most, line), half),
            pltpu.VMEM((count, FLUXES * most, line), half),
            pltpu.VMEM((count, 1, line), full),
            pltpu.VMEM((count, 1, line), full),
            pltpu.VMEM((count, SLOTS, line), half),
            pltpu.VMEM((count, SLOTS, line), half),
            pltpu.VMEM((4, MARINE_STRATA, line), full),
            pltpu.VMEM((4, MARINE_STRATA, line), full),
            pltpu.VMEM((MARINE_STRATA, OX + 16, line), full),
            pltpu.VMEM((2 + MARINE_STRATA, OX, line), full),
            pltpu.VMEM((OX + 16, line), full),
            pltpu.VMEM((3, 2, TALL, line), full),
            pltpu.VMEM((3, 2, TALL, line), full),
            pltpu.VMEM((2, TALL, line), full),
        ]
        + boxes(4)
        + [pltpu.VMEM((2, OX, line), half), pltpu.VMEM((2, FRAME, line), half)]
        + boxes(3)
        + boxes(3)
        + [pltpu.SemaphoreType.DMA((3 + PARTS + 5,))]
        + [pltpu.SemaphoreType.DMA((count,))] * 6
        + [pltpu.SemaphoreType.DMA((4,))] * 2
        + [pltpu.SemaphoreType.DMA((8,))] * 8,
        compiler_params=pltpu.CompilerParams(
            collective_id=0, has_side_effects=True, vmem_limit_bytes=24 * 1024 * 1024
        ),
        name="window",
    )(
        *[
            pltpu.with_memory_space_constraint(value, pltpu.HBM)
            for value in (
                sky_interface_transfers,
                coupling_matrix_enlarged,
                piece_keeper_part.reshape(1, NB),
                receiving_part_line,
                marine_point_switch,
                potential_heat_deviation,
                free_marine_lift,
                depth_averaged_uflow,
                depth_averaged_vflow,
            )
        ]
    )
    anywhere = pl.BlockSpec(memory_space=pl.ANY)
    return pl.pallas_call(
        hand_over,
        out_shape=shapes,
        in_specs=[anywhere] * 3,
        out_specs=(anywhere,) * 3,
        scratch_shapes=[pltpu.VMEM(shape.shape, jnp.float32) for shape in shapes]
        + [pltpu.SemaphoreType.DMA((3,))] * 2,
        compiler_params=pltpu.CompilerParams(vmem_limit_bytes=8 * 1024 * 1024),
        name="hand_over",
    )(*results)


def solution(mesh):
    in_specs = (
        P(None, "gy", "gx"),
        P("gy", "gx", None),
        P("gx", "gy", None),
        P("gx", "gy"),
        P("gx", "gy"),
        P(None, "gx", "gy"),
        P("gx", "gy"),
        P("gx", "gy"),
        P("gx", "gy"),
    )
    out_specs = (P("gy", "gx"), P(None, "gx", "gy"), P(None, "gx", "gy"))
    return jax.shard_map(
        per_device, mesh=mesh, in_specs=in_specs, out_specs=out_specs, check_vma=False
    )
```

```python
import jax
import jax.numpy as jnp
from jax import lax
from jax.experimental import pallas as pl
from jax.experimental.pallas import tpu as pltpu
from jax.sharding import PartitionSpec as P

NB = 96
OX = 128
BAND_NORTH_COUNT = 128
MARINE_STRATA = 8
SUB = 40


HORIZ_MIX = 0.15
VERT_MIX = 0.2
HEAT_GAIN = 0.5
FLOW_DAMP = 0.98
PRESS_GAIN = 0.6
DIVERGE_GAIN = 0.6
CORIOLIS = 0.1
WIND_GAIN = 0.05
FRESH_GAIN = 0.05


MESH = pl.DeviceIdType.MESH
LANES = BAND_NORTH_COUNT
HALF = LANES // 2
SPAN = SUB // 2
MARGIN = 2 * SPAN
BASE = MARGIN + 8
TALL = OX + 2 * BASE
FRAME = OX + 2 * MARGIN
OVERLAP = (LANES - 2 * MARGIN) // 2
GROUP = 4
RENEW = 3 * GROUP
CHUNK = 16
SLOTS = 8
FLUXES = 4
PARTS = 4
EDGES = 16
HEIGHT_EDGE = MARINE_STRATA
WET_EDGE = MARINE_STRATA + 1


def turn_lanes(values, shift):
    shift = shift % LANES
    return pltpu.roll(values, shift, 1) if shift else values


def lanes(rows):
    return lax.broadcasted_iota(jnp.int32, (rows, LANES), 1)


def neighbours():
    nx, ny = lax.axis_size("gx"), lax.axis_size("gy")
    x, y = lax.axis_index("gx"), lax.axis_index("gy")
    up, down = lax.rem(x + 1, nx), lax.rem(x + nx - 1, nx)
    right, left = lax.rem(y + 1, ny), lax.rem(y + ny - 1, ny)
    return x, y, up, down, right, left


def peer_place(index):
    ny = lax.axis_size("gy")
    return lax.div(index, ny), lax.rem(index, ny)


def greet_all(me, count):
    barrier = pltpu.get_barrier_semaphore()

    def one(k, carry):
        place = peer_place(lax.rem(me + k, count))
        pl.semaphore_signal(barrier, inc=1, device_id=place, device_id_type=MESH)
        return carry

    lax.fori_loop(1, count, one, 0)


def peers(action, out, into, send_sem, recv_sem):
    nx, ny = lax.axis_size("gx"), lax.axis_size("gy")
    x, y = lax.axis_index("gx"), lax.axis_index("gy")
    me = x * ny + y
    for dy in sorted(range(ny), key=lambda d: abs(2 * d - ny)):

        def one(dx, carry, dy=dy):
            to_x, to_y = lax.rem(x + dx, nx), lax.rem(y + dy, ny)
            copy = pltpu.make_async_remote_copy(
                src_ref=out.at[to_x * ny + to_y],
                dst_ref=into.at[me],
                send_sem=send_sem.at[dx * ny + dy],
                recv_sem=recv_sem.at[dx * ny + dy],
                device_id=(to_x, to_y),
                device_id_type=MESH,
            )
            if action == "start":
                copy.start()
            else:
                copy.wait()
            return carry

        lax.fori_loop(0 if dy else 1, nx, one, 0, unroll=True)


def as_bits(condition):
    return jnp.where(condition, 1.0, 0.0).astype(jnp.bfloat16)


def line_numbers(shape, axis):
    return lax.broadcasted_iota(jnp.int32, shape, axis).astype(jnp.float32)


def dot(a, b, a_dim=1, b_dim=0):
    return lax.dot_general(
        a, b, (((a_dim,), (b_dim,)), ((), ())), preferred_element_type=jnp.float32
    )


def place_blocks(keeper, lines, count):
    i, j = line_numbers((NB, NB), 0), line_numbers((NB, NB), 1)
    owner_row = keeper[...].astype(jnp.float32)
    owner_col = jnp.sum(jnp.where(i == j, owner_row, 0.0), axis=1, keepdims=True)
    same = jnp.where(owner_col == owner_row, 1.0, 0.0)
    rank_row = jnp.sum(jnp.where(i < j, same, 0.0), axis=0, keepdims=True)
    rank_col = jnp.sum(jnp.where(j < i, same, 0.0), axis=1, keepdims=True)
    line_row = lines[...].astype(jnp.float32)
    line_col = jnp.sum(jnp.where(i == j, line_row, 0.0), axis=1, keepdims=True)
    owned = as_bits(line_numbers((count, NB), 0) == owner_row)
    ranked = jnp.where(line_numbers((NB, LANES), 1) == rank_col, line_col + 1.0, 0.0)
    listed = dot(owned, ranked.astype(jnp.bfloat16))
    return owner_row * SLOTS + rank_row, owner_col * SLOTS + rank_col, listed


def regrid(sky, weights, partial, waits):
    slot32 = lax.rem(lax.broadcasted_iota(jnp.int32, (FLUXES * SLOTS, LANES), 0), SLOTS)
    groups = NB // SLOTS
    for g in range(groups):
        if g % (groups // PARTS) == 0:
            waits[g // (groups // PARTS)].wait()
        rows = slice(g * SLOTS, (g + 1) * SLOTS)
        fluxes = sky[:, rows, :].astype(jnp.float32).reshape(FLUXES * SLOTS, OX)
        fluxes = fluxes.astype(jnp.bfloat16)
        total = dot(fluxes, weights[g * SLOTS])
        for n in range(1, SLOTS):
            total = jnp.where(slot32 == n, dot(fluxes, weights[g * SLOTS + n]), total)
        partial[:, rows, :] = total.reshape(FLUXES, SLOTS, LANES)


def fill_send(send, stage, partial, slots, count, most):
    rows = FLUXES * most
    pairs = []
    for f in range(0, FLUXES, 2):
        both = jnp.concatenate([partial[f], partial[f + 1]], axis=1).astype(jnp.bfloat16)
        pairs.append(dot(slots, both))
    for d in range(count):
        for f in range(FLUXES):
            at = d * rows + f * most
            from_lane = (f % 2) * LANES
            stage[at : at + SLOTS] = pairs[f // 2][
                d * SLOTS : (d + 1) * SLOTS, from_lane : from_lane + LANES
            ]
    send[...] = stage[0 : count * rows].reshape(count, rows, LANES).astype(jnp.bfloat16)


def read_targets(listed_in, count):
    lane = line_numbers((SLOTS, LANES), 1)
    row = line_numbers((SLOTS, LANES), 0)
    tiles = []
    for s in range(count):
        line = jnp.broadcast_to(listed_in[s], (SLOTS, LANES))
        line = jnp.sum(jnp.where(lane == row, line, 0.0), axis=1, keepdims=True)
        tiles.append(jnp.where(lane + 1.0 == line, 1.0, 0.0))
    return jnp.concatenate(tiles, axis=0)


def read_fluxes(recv, stage, count, most):
    rows = FLUXES * most
    stage[0 : count * rows] = recv[...].astype(jnp.float32).reshape(count * rows, LANES)
    values = []
    for f in range(FLUXES):
        starts = [s * rows + f * most for s in range(count)]
        tiles = [stage[at : at + SLOTS] for at in starts]
        values.append(jnp.concatenate(tiles, axis=0).astype(jnp.bfloat16))
    return values


def edge_selector(rows, low_row, high_row):
    row = lax.broadcasted_iota(jnp.int32, (rows, BAND_NORTH_COUNT), 0)
    lane = lax.broadcasted_iota(jnp.int32, (rows, BAND_NORTH_COUNT), 1)
    return as_bits(
        ((row == low_row) & (lane == 0)) | ((row == high_row) & (lane == BAND_NORTH_COUNT - 1))
    )


def fill_edges(heat, height, wet, edges):
    selector = edge_selector(8, 0, 1)
    blank = jnp.zeros((EDGES - MARINE_STRATA, LANES), jnp.float32)
    for end in range(4):
        edges[end, MARINE_STRATA:EDGES] = blank
    fields = [heat[k] for k in range(MARINE_STRATA)] + [height, wet]
    for k, values in enumerate(fields):
        row = slice(k, k + 1)
        edges[0, row] = values[0:1]
        edges[1, row] = values[OX - 1 : OX]
        sides = dot(selector, values.astype(jnp.bfloat16), 1, 1)
        edges[2, row] = sides[0:1]
        edges[3, row] = sides[1:2]


def heat_copies(edges, got, send_sem, recv_sem):
    x, y, up, down, right, left = neighbours()
    plan = ((1, 0, (up, y)), (0, 1, (down, y)), (3, 2, (x, right)), (2, 3, (x, left)))
    return [
        pltpu.make_async_remote_copy(
            src_ref=edges.at[src],
            dst_ref=got.at[dst],
            send_sem=send_sem.at[k],
            recv_sem=recv_sem.at[k],
            device_id=place,
            device_id_type=MESH,
        )
        for k, (src, dst, place) in enumerate(plan)
    ]


def heat_step(heat, got, tall, shore, near, out):
    last = lanes(OX) == LANES - 1
    first = lanes(OX) == 0
    mine = shore[8 : 8 + OX]
    sides = jnp.concatenate([got[3], got[2]], axis=0).astype(jnp.bfloat16)
    wet = dot(sides, edge_selector(2 * EDGES, EDGES + WET_EDGE, WET_EDGE), 0, 0)
    near[0] = jnp.where(last, wet, turn_lanes(mine, -1))
    near[1] = jnp.where(first, wet, turn_lanes(mine, 1))
    for k in range(MARINE_STRATA):
        tall[k, 8 : 8 + OX] = heat[k]
        tall[k, 7:8] = got[0, k : k + 1]
        tall[k, 8 + OX : 9 + OX] = got[1, k : k + 1]
        near[2 + k] = dot(sides, edge_selector(2 * EDGES, EDGES + k, k), 0, 0)

    step = 32
    last, first = last[:step], first[:step]

    def one(k, carry):
        above, below = jnp.maximum(k - 1, 0), jnp.minimum(k + 1, MARINE_STRATA - 1)
        for start in range(0, OX, step):
            rows = slice(start, start + step)
            tall_rows = lambda shift: slice(8 + start + shift, 8 + start + step + shift)
            here = heat[k, rows]
            side = near[2 + k, rows]
            north = jnp.where(last, side, turn_lanes(here, -1))
            south = jnp.where(first, side, turn_lanes(here, 1))
            lateral = shore[tall_rows(1)] * (tall[k, tall_rows(1)] - here)
            lateral = lateral + shore[tall_rows(-1)] * (tall[k, tall_rows(-1)] - here)
            lateral = lateral + near[0, rows] * (north - here)
            lateral = lateral + near[1, rows] * (south - here)
            vertical = (heat[above, rows] - here) + (heat[below, rows] - here)
            out[k, rows] = (here + HORIZ_MIX * lateral + VERT_MIX * vertical) * shore[tall_rows(0)]
        return carry

    lax.fori_loop(0, MARINE_STRATA, one, 0)


def remote(src, dst, place, send, recv, k):
    return pltpu.make_async_remote_copy(
        src_ref=src,
        dst_ref=dst,
        send_sem=send.at[k],
        recv_sem=recv.at[k],
        device_id=place,
        device_id_type=MESH,
    )


class Exchange:
    def __init__(self, rows, edge, packs, sides, send, recv):
        x, y, up, down, right, left = neighbours()
        ny = lax.axis_size("gy")
        low, high = packs.at[0], packs.at[1]
        from_left, from_right = sides.at[0], sides.at[1]
        top, whole, bottom = pl.ds(OX - MARGIN, MARGIN), pl.ds(0, OX), pl.ds(0, MARGIN)
        before, middle, after = pl.ds(0, MARGIN), pl.ds(MARGIN, OX), pl.ds(MARGIN + OX, MARGIN)
        moves = ((top, before, up), (bottom, after, down), (whole, middle, x))
        self.rows = []
        if rows is not None:
            self.rows = [
                remote(rows.at[1], edge.at[0], (up, y), send, recv, 6),
                remote(rows.at[0], edge.at[1], (down, y), send, recv, 7),
            ]
        self.right = [
            remote(high.at[src], from_left.at[dst], (to, right), send, recv, k)
            for k, (src, dst, to) in enumerate(moves)
        ]
        self.left = [
            remote(low.at[src], from_right.at[dst], (to, left), send, recv, 3 + k)
            for k, (src, dst, to) in enumerate(moves)
        ]
        self.has_right, self.has_left = y < ny - 1, y > 0

    def guarded(self, condition, copies, action):
        def act():
            for copy in copies:
                getattr(copy, action)()

        pl.when(condition)(act)

    def start(self):
        self.guarded(self.has_right, self.right, "start")
        self.guarded(self.has_left, self.left, "start")
        for copy in self.rows:
            copy.start()

    def wait(self):
        for copy in self.rows:
            copy.wait()
        self.guarded(self.has_left, self.right, "wait_recv")
        self.guarded(self.has_right, self.left, "wait_recv")
        self.guarded(self.has_right, self.right, "wait_send")
        self.guarded(self.has_left, self.left, "wait_send")


def clear_walls(sides):
    y, ny = lax.axis_index("gy"), lax.axis_size("gy")
    blank = jnp.zeros((FRAME, LANES), jnp.bfloat16)

    @pl.when(y == 0)
    def _():
        for side in sides:
            side[0] = blank

    @pl.when(y == ny - 1)
    def _():
        for side in sides:
            side[1] = blank


def fill_rows(rows, field, values):
    rows[0, field] = values[:MARGIN].astype(jnp.bfloat16)
    rows[1, field] = values[OX - MARGIN :].astype(jnp.bfloat16)


def fill_packs(packs, values):
    lane = lanes(OX)
    low = turn_lanes(values[2], LANES - 3 * MARGIN)
    low = jnp.where(lane >= LANES - 2 * MARGIN, turn_lanes(values[1], LANES - 2 * MARGIN), low)
    low = jnp.where(lane >= LANES - MARGIN, turn_lanes(values[0], LANES - MARGIN), low)
    high = turn_lanes(values[2], 3 * MARGIN)
    high = jnp.where(lane < 2 * MARGIN, turn_lanes(values[1], 2 * MARGIN), high)
    high = jnp.where(lane < MARGIN, turn_lanes(values[0], MARGIN), high)
    packs[0] = low.astype(jnp.bfloat16)
    packs[1] = high.astype(jnp.bfloat16)


def zones():
    return (
        (BASE - MARGIN, 0, MARGIN, 0),
        (BASE, MARGIN, OX, None),
        (BASE + OX, MARGIN + OX, MARGIN, 1),
    )


def spread_fields(natural, edge, sides, wide, mask):
    for at, side_at, size, end in zones():
        lane = lanes(size)
        here, there = slice(at, at + size), slice(side_at, side_at + size)
        from_left = sides[0, there].astype(jnp.float32)
        from_right = sides[1, there].astype(jnp.float32)
        for f in range(3):
            centre = natural[f] if end is None else edge[end, f].astype(jnp.float32)
            left = turn_lanes(from_left, -f * MARGIN)
            right = turn_lanes(from_right, f * MARGIN)
            one = jnp.where(lane < MARGIN, left, turn_lanes(centre, MARGIN))
            two = jnp.where(lane >= LANES - MARGIN, right, turn_lanes(centre, -MARGIN))
            if mask is not None and f > 0:
                one = jnp.where(mask[0, here] > 0, one, 0.0)
                two = jnp.where(mask[1, here] > 0, two, 0.0)
            wide[f, 0, here] = one
            wide[f, 1, here] = two


def spread_wet(shore, edge, sides, gain):
    for at, side_at, size, end in zones():
        lane = lanes(size)
        here, there = slice(at, at + size), slice(side_at, side_at + size)
        from_left = sides[0, there].astype(jnp.float32)
        from_right = sides[1, there].astype(jnp.float32)
        centre = shore[8 : 8 + OX] if end is None else edge[end, 3].astype(jnp.float32)
        one = jnp.where(lane >= LANES - MARGIN, from_left, centre)
        two = jnp.where(lane < MARGIN, from_right, centre)
        gain[0, here] = PRESS_GAIN * turn_lanes(one, MARGIN)
        gain[1, here] = PRESS_GAIN * turn_lanes(two, -MARGIN)


def height_over_wall(got, state):
    y, ny = lax.axis_index("gy"), lax.axis_size("gy")
    row = lax.broadcasted_iota(jnp.int32, (2 * EDGES, LANES), 0)
    lane = lanes(2 * EDGES)
    low = (row == EDGES + HEIGHT_EDGE) & (lane == MARGIN - 1)
    high = (row == HEIGHT_EDGE) & (lane == LANES - MARGIN)
    sides = jnp.concatenate([got[3], got[2]], axis=0).astype(jnp.bfloat16)
    values = dot(sides, as_bits(low | high), 0, 0)
    rows, lane = slice(BASE, BASE + OX), lanes(OX)

    @pl.when(y == 0)
    def _():
        state[0, 0, rows] = jnp.where(lane == MARGIN - 1, values, state[0, 0, rows])

    @pl.when(y == ny - 1)
    def _():
        state[0, 1, rows] = jnp.where(lane == LANES - MARGIN, values, state[0, 1, rows])


def renew_overlap(state, reach):
    low, high = BASE - reach, BASE + OX + reach
    shift = LANES - 2 * MARGIN + 2 * OVERLAP
    for start in range(low, high, CHUNK):
        rows = slice(start, start + CHUNK)
        lane = lanes(CHUNK)
        for f in range(3):
            one, two = state[f, 0, rows], state[f, 1, rows]
            state[f, 0, rows] = jnp.where(lane >= LANES - OVERLAP, turn_lanes(two, 2 * MARGIN), one)
            state[f, 1, rows] = jnp.where(lane < OVERLAP, turn_lanes(one, -2 * MARGIN), two)


def own_part(state, f, rows=None):
    one, two = state[f, 0, BASE : BASE + OX], state[f, 1, BASE : BASE + OX]
    return jnp.where(lanes(OX) < HALF, turn_lanes(one, -MARGIN), turn_lanes(two, MARGIN))


def substep(reach, state, forces, gain, turning, raw):
    low, high = BASE - reach, BASE + OX + reach
    turn = [jnp.broadcast_to(turning[tile : tile + 1, :], (CHUNK, LANES)) for tile in range(2)]

    def velocity(start, tile):
        rows = slice(start, start + CHUNK)
        height = state[0, tile, rows]
        slope_east = (
            state[0, tile, start + 1 : start + CHUNK + 1]
            - state[0, tile, start - 1 : start + CHUNK - 1]
        )
        slope_north = turn_lanes(height, -1) - turn_lanes(height, 1)
        old_u, old_v, slope = state[1, tile, rows], state[2, tile, rows], gain[tile, rows]
        new_u = (FLOW_DAMP * old_u + turn[tile] * old_v) + (
            forces[0, tile, rows] - slope * slope_east
        )
        new_v = (FLOW_DAMP * old_v + (forces[1, tile, rows] - slope * slope_north)) - (
            turn[tile] * new_u
        )
        state[1, tile, rows] = new_u
        state[2, tile, rows] = new_v

    def surface(start, tile):
        rows = slice(start, start + CHUNK)
        flow_north = state[2, tile, rows]
        spread_east = (
            state[1, tile, start + 1 : start + CHUNK + 1]
            - state[1, tile, start - 1 : start + CHUNK - 1]
        )
        spread_north = turn_lanes(flow_north, -1) - turn_lanes(flow_north, 1)
        height, slope = state[0, tile, rows], gain[tile, rows]
        if raw:
            height = jnp.where(slope > 0, height, 0.0)
        state[0, tile, rows] = (height - forces[2, tile, rows]) - slope * (
            spread_east + spread_north
        )

    starts = range(low, high, CHUNK)
    for start in starts:
        for tile in range(2):
            velocity(start, tile)
    for start in starts:
        for tile in range(2):
            surface(start, tile)


def run_span(state, forces, gain, turning, raw):
    done = 0
    while done < SPAN:
        need = 2 * (SPAN - done) - 1
        reach = -(-need // 8) * 8
        steps = min(SPAN - done, GROUP)
        if done == RENEW:
            renew_overlap(state, reach)
        if raw and done == 0:
            substep(reach, state, forces, gain, turning, True)

        def one(_, carry, reach=reach):
            substep(reach, state, forces, gain, turning, False)
            return carry

        lax.fori_loop(1 if raw and done == 0 else 0, steps, one, 0, unroll=True)
        done += steps


def window_kernel(
    sky_far, weights_far, keeper_far, lines_far, sea_far, heat_far, h_far, u_far, v_far,
    back, heat_out, out,
    sky, weights, keeper, lines, sea, heat, natural,
    turning, partial, stage, send, recv, listed_out, listed_in, skin_send, skin_recv,
    heat_edges, heat_got, tall, near, shore,
    state, forces, gain,
    rows1, edge1, packs1, sides1, wets, wets_in,
    rows2, edge2, packs2, sides2, rows3, edge3, packs3, sides3,
    load_sem, list_send, list_recv, a2a_send, a2a_recv, skin_send_sem, skin_recv_sem,
    heat_send_sem, heat_recv_sem, send0, recv0, send1, recv1, send2, recv2, send3, recv3,
):
    ny = lax.axis_size("gy")
    count = lax.axis_size("gx") * ny
    most = max(2, 2 * NB // count)
    me = lax.axis_index("gx") * ny + lax.axis_index("gy")
    part = NB // PARTS
    pieces = [pl.ds(p * part, part) for p in range(PARTS)]
    moves = [(keeper_far, keeper), (lines_far, lines), (sky_far, sky)]
    moves += [(weights_far.at[pieces[0]], weights.at[pieces[0]])]
    moves += [(sea_far, sea), (h_far, natural.at[0]), (heat_far, heat)]
    moves += [(weights_far.at[piece], weights.at[piece]) for piece in pieces[1:]]
    moves += [(u_far, natural.at[1]), (v_far, natural.at[2])]
    loads = [
        pltpu.make_async_copy(src, dst, load_sem.at[k]) for k, (src, dst) in enumerate(moves)
    ]
    for load in loads:
        load.start()
    greet_all(me, count)
    turning[...] = turning_rows()
    clear_walls((sides1, sides2, sides3, wets_in))
    blank = jnp.zeros((8, LANES), jnp.float32)
    for f in range(2):
        for tile in range(2):
            state[f, tile, BASE - MARGIN - 8 : BASE - MARGIN] = blank
            state[f, tile, BASE + OX + MARGIN : BASE + OX + MARGIN + 8] = blank
    stage[count * FLUXES * most : count * FLUXES * most + SLOTS] = blank
    loads[0].wait()
    loads[1].wait()
    key_row, key_col, listed = place_blocks(keeper, lines, count)
    for d in range(count):
        listed_out[d] = listed[d : d + 1]
    slots = as_bits(line_numbers((count * SLOTS, NB), 0) == key_row)
    for load in loads[4:7]:
        load.wait()
    lat = lax.axis_index("gy") * LANES + lanes(OX)
    inside = (lat > 0) & (lat < ny * LANES - 1)
    shore[8 : 8 + OX] = jnp.where(inside, sea[...].astype(jnp.float32), 0.0)
    fill_edges(heat, natural[0], shore[8 : 8 + OX], heat_edges)
    heats = heat_copies(heat_edges, heat_got, heat_send_sem, heat_recv_sem)
    loads[2].wait()
    regrid(sky, weights, partial, [loads[3]] + loads[7 : 6 + PARTS])
    fill_send(send, stage, partial, slots, count, most)
    pl.semaphore_wait(pltpu.get_barrier_semaphore(), count - 1)
    for copy in heats:
        copy.start()
    peers("start", listed_out, listed_in, list_send, list_recv)
    peers("start", send, recv, a2a_send, a2a_recv)
    recv[me] = send[me]
    listed_in[me] = listed_out[me]
    for load in loads[6 + PARTS :]:
        load.wait()
    for f in range(3):
        fill_rows(rows1, f, natural[f])
    fill_rows(rows1, 3, shore[8 : 8 + OX])
    fill_packs(packs1, [natural[f] for f in range(3)])
    wets[0] = shore[8 : 8 + OX].astype(jnp.bfloat16)
    wets[1] = shore[8 : 8 + OX].astype(jnp.bfloat16)
    first = Exchange(rows1, edge1, packs1, sides1, send1, recv1)
    wet = Exchange(None, None, wets, wets_in, send0, recv0)
    wet.start()
    first.start()
    for copy in heats:
        copy.wait()
    shore[7:8] = heat_got[0, WET_EDGE : WET_EDGE + 1]
    shore[8 + OX : 9 + OX] = heat_got[1, WET_EDGE : WET_EDGE + 1]
    heat_step(heat, heat_got, tall, shore, near, heat_out)
    peers("wait", listed_out, listed_in, list_send, list_recv)
    target = read_targets(listed_in, count)
    target_turned = target.T.astype(jnp.bfloat16)
    target = target.astype(jnp.bfloat16)
    peers("wait", send, recv, a2a_send, a2a_recv)
    values = read_fluxes(recv, stage, count, most)
    stress = dot(target_turned, jnp.concatenate([values[0], values[1]], axis=1))
    others = dot(target_turned, jnp.concatenate([values[3], values[2]], axis=1))
    mask = shore[8 : 8 + OX]
    own = [
        WIND_GAIN * stress[:, :LANES] * mask,
        WIND_GAIN * stress[:, LANES:] * mask,
        FRESH_GAIN * others[:, :LANES] * mask,
    ]
    for f in range(3):
        fill_rows(rows2, f, own[f])
    fill_packs(packs2, own)
    second = Exchange(rows2, edge2, packs2, sides2, send2, recv2)
    second.start()
    wet.wait()
    first.wait()
    spread_wet(shore, edge1, wets_in, gain)
    spread_fields(natural, edge1, sides1, state, gain)
    height_over_wall(heat_got, state)
    surface = heat_out[0] + HEAT_GAIN * others[:, LANES:] * shore[8 : 8 + OX]
    heat_out[0] = surface
    band = dot(target, surface.astype(jnp.bfloat16))
    skin_send[...] = band.reshape(count, SLOTS, LANES).astype(jnp.bfloat16)
    peers("start", skin_send, skin_recv, skin_send_sem, skin_recv_sem)
    skin_recv[me] = skin_send[me]
    second.wait()
    spread_fields(own, edge2, sides2, forces, None)
    run_span(state, forces, gain, turning, True)
    for f in range(3):
        natural[f] = own_part(state, f)
        fill_rows(rows3, f, natural[f])
    fill_packs(packs3, [natural[f] for f in range(3)])
    third = Exchange(rows3, edge3, packs3, sides3, send3, recv3)
    third.start()
    peers("wait", skin_send, skin_recv, skin_send_sem, skin_recv_sem)
    slots = as_bits(line_numbers((NB, count * SLOTS), 1) == key_col)
    skin = dot(slots, skin_recv[...].reshape(count * SLOTS, LANES))
    slot8 = lax.broadcasted_iota(jnp.int32, (SLOTS, LANES), 0)
    for g in range(NB // SLOTS):
        rows = slice(g * SLOTS, (g + 1) * SLOTS)
        lines_skin = skin[rows].astype(jnp.bfloat16)
        total = dot(lines_skin, weights[g * SLOTS], 1, 1)
        for n in range(1, SLOTS):
            total = jnp.where(slot8 == n, dot(lines_skin, weights[g * SLOTS + n], 1, 1), total)
        back[rows] = total
    third.wait()
    spread_fields(natural, edge3, sides3, state, None)
    run_span(state, forces, gain, turning, False)
    for f in range(3):
        out[f] = own_part(state, f)


def turning_rows():
    total_y = lax.axis_size("gy") * LANES
    shape = (8, LANES)
    lane = lax.broadcasted_iota(jnp.int32, shape, 1)
    tile = lax.broadcasted_iota(jnp.int32, shape, 0)
    rows = lax.axis_index("gy") * LANES + lane + jnp.where(tile == 0, -MARGIN, MARGIN)
    rows = jnp.where(rows < 0, rows + total_y, jnp.where(rows < total_y, rows, rows - total_y))
    return CORIOLIS * jnp.sin(jnp.pi * ((rows.astype(jnp.float32) + 0.5) / total_y - 0.5))


def hand_over(*refs):
    sources, targets = refs[:3], refs[3:6]
    buffers, loads, stores = refs[6:9], refs[9], refs[10]
    into = [
        pltpu.make_async_copy(sources[k], buffers[k], loads.at[k]) for k in range(3)
    ]
    away = [
        pltpu.make_async_copy(buffers[k], targets[k], stores.at[k]) for k in range(3)
    ]
    for copy in into:
        copy.start()
    for k in range(3):
        into[k].wait()
        away[k].start()
    for copy in away:
        copy.wait()


def per_device(
    sky_interface_transfers,
    coupling_matrix_enlarged,
    piece_keeper_part,
    receiving_part_line,
    marine_point_switch,
    potential_heat_deviation,
    free_marine_lift,
    depth_averaged_uflow,
    depth_averaged_vflow,
):
    count = lax.axis_size("gx") * lax.axis_size("gy")
    most = max(2, 2 * NB // count)
    line = LANES
    half = jnp.bfloat16
    full = jnp.float32

    def boxes(fields):
        return [
            pltpu.VMEM((2, fields, MARGIN, line), half),
            pltpu.VMEM((2, fields, MARGIN, line), half),
            pltpu.VMEM((2, OX, line), half),
            pltpu.VMEM((2, FRAME, line), half),
        ]

    inside = pl.BlockSpec(memory_space=pltpu.VMEM)
    far = pl.BlockSpec(memory_space=pltpu.HBM)
    shapes = (
        jax.ShapeDtypeStruct((NB, OX), full),
        jax.ShapeDtypeStruct((MARINE_STRATA, OX, line), full),
        jax.ShapeDtypeStruct((3, OX, line), full),
    )
    results = pl.pallas_call(
        window_kernel,
        out_shape=shapes,
        in_specs=[far] * 9,
        out_specs=(inside,) * 3,
        scratch_shapes=[
            pltpu.VMEM((FLUXES, NB, OX), half),
            pltpu.VMEM((NB, OX, line), half),
            pltpu.VMEM((1, NB), jnp.int32),
            pltpu.VMEM((1, NB), jnp.int32),
            pltpu.VMEM((OX, line), jnp.int32),
            pltpu.VMEM((MARINE_STRATA, OX, line), full),
            pltpu.VMEM((3, OX, line), full),
            pltpu.VMEM((8, line), full),
            pltpu.VMEM((FLUXES, NB, line), full),
            pltpu.VMEM((count * FLUXES * most + SLOTS, line), full),
            pltpu.VMEM((count, FLUXES * most, line), half),
            pltpu.VMEM((count, FLUXES * most, line), half),
            pltpu.VMEM((count, 1, line), full),
            pltpu.VMEM((count, 1, line), full),
            pltpu.VMEM((count, SLOTS, line), half),
            pltpu.VMEM((count, SLOTS, line), half),
            pltpu.VMEM((4, EDGES, line), full),
            pltpu.VMEM((4, EDGES, line), full),
            pltpu.VMEM((MARINE_STRATA, OX + 16, line), full),
            pltpu.VMEM((2 + MARINE_STRATA, OX, line), full),
            pltpu.VMEM((OX + 16, line), full),
            pltpu.VMEM((3, 2, TALL, line), full),
            pltpu.VMEM((3, 2, TALL, line), full),
            pltpu.VMEM((2, TALL, line), full),
        ]
        + boxes(4)
        + [pltpu.VMEM((2, OX, line), half), pltpu.VMEM((2, FRAME, line), half)]
        + boxes(3)
        + boxes(3)
        + [pltpu.SemaphoreType.DMA((3 + PARTS + 5,))]
        + [pltpu.SemaphoreType.DMA((count,))] * 6
        + [pltpu.SemaphoreType.DMA((4,))] * 2
        + [pltpu.SemaphoreType.DMA((8,))] * 8,
        compiler_params=pltpu.CompilerParams(
            collective_id=0, has_side_effects=True, vmem_limit_bytes=24 * 1024 * 1024
        ),
        name="window",
    )(
        *[
            pltpu.with_memory_space_constraint(value, pltpu.HBM)
            for value in (
                sky_interface_transfers,
                coupling_matrix_enlarged,
                piece_keeper_part.reshape(1, NB),
                receiving_part_line,
                marine_point_switch,
                potential_heat_deviation,
                free_marine_lift,
                depth_averaged_uflow,
                depth_averaged_vflow,
            )
        ]
    )
    anywhere = pl.BlockSpec(memory_space=pl.ANY)
    return pl.pallas_call(
        hand_over,
        out_shape=shapes,
        in_specs=[anywhere] * 3,
        out_specs=(anywhere,) * 3,
        scratch_shapes=[pltpu.VMEM(shape.shape, jnp.float32) for shape in shapes]
        + [pltpu.SemaphoreType.DMA((3,))] * 2,
        compiler_params=pltpu.CompilerParams(vmem_limit_bytes=8 * 1024 * 1024),
        name="hand_over",
    )(*results)


def solution(mesh):
    in_specs = (
        P(None, "gy", "gx"),
        P("gy", "gx", None),
        P("gx", "gy", None),
        P("gx", "gy"),
        P("gx", "gy"),
        P(None, "gx", "gy"),
        P("gx", "gy"),
        P("gx", "gy"),
        P("gx", "gy"),
    )
    out_specs = (P("gy", "gx"), P(None, "gx", "gy"), P(None, "gx", "gy"))
    return jax.shard_map(
        per_device, mesh=mesh, in_specs=in_specs, out_specs=out_specs, check_vma=False
    )
```

```python
import jax
import jax.numpy as jnp
from jax import lax
from jax.experimental import pallas as pl
from jax.experimental.pallas import tpu as pltpu
from jax.sharding import PartitionSpec as P

NB = 96
OX = 128
BAND_NORTH_COUNT = 128
MARINE_STRATA = 8
SUB = 40


HORIZ_MIX = 0.15
VERT_MIX = 0.2
HEAT_GAIN = 0.5
FLOW_DAMP = 0.98
PRESS_GAIN = 0.6
DIVERGE_GAIN = 0.6
CORIOLIS = 0.1
WIND_GAIN = 0.05
FRESH_GAIN = 0.05


MESH = pl.DeviceIdType.MESH
LANES = BAND_NORTH_COUNT
HALF = LANES // 2
SPAN = SUB // 2
MARGIN = 2 * SPAN
BASE = MARGIN + 8
TALL = OX + 2 * BASE
FRAME = OX + 2 * MARGIN
OVERLAP = (LANES - 2 * MARGIN) // 2
GROUP = 4
RENEW = 3 * GROUP
CHUNK = 16
SLOTS = 8
FLUXES = 4
PARTS = 4
EDGES = 16
HEIGHT_EDGE = MARINE_STRATA
WET_EDGE = MARINE_STRATA + 1


def turn_lanes(values, shift):
    shift = shift % LANES
    return pltpu.roll(values, shift, 1) if shift else values


def lanes(rows):
    return lax.broadcasted_iota(jnp.int32, (rows, LANES), 1)


def neighbours():
    nx, ny = lax.axis_size("gx"), lax.axis_size("gy")
    x, y = lax.axis_index("gx"), lax.axis_index("gy")
    up, down = lax.rem(x + 1, nx), lax.rem(x + nx - 1, nx)
    right, left = lax.rem(y + 1, ny), lax.rem(y + ny - 1, ny)
    return x, y, up, down, right, left


def far_first(act):
    nx, ny = lax.axis_size("gx"), lax.axis_size("gy")
    x, y = lax.axis_index("gx"), lax.axis_index("gy")
    for dy in sorted(range(ny), key=lambda d: abs(2 * d - ny)):

        def one(dx, carry, dy=dy):
            act(lax.rem(x + dx, nx), lax.rem(y + dy, ny))
            return carry

        lax.fori_loop(0 if dy else 1, nx, one, 0, unroll=True)


def greet_all():
    barrier = pltpu.get_barrier_semaphore()

    def greet(to_x, to_y):
        pl.semaphore_signal(barrier, inc=1, device_id=(to_x, to_y), device_id_type=MESH)

    far_first(greet)


def remote(src, dst, place, send_sem, recv_sem):
    return pltpu.make_async_remote_copy(
        src_ref=src,
        dst_ref=dst,
        send_sem=send_sem,
        recv_sem=recv_sem,
        device_id=place,
        device_id_type=MESH,
    )


class Swap:
    def __init__(self, out, into, send_sem, recv_sem):
        self.out, self.into, self.sems = out, into, (send_sem, recv_sem)

    def start(self):
        ny = lax.axis_size("gy")
        me = lax.axis_index("gx") * ny + lax.axis_index("gy")

        def send(to_x, to_y):
            place = (to_x, to_y)
            remote(self.out.at[to_x * ny + to_y], self.into.at[me], place, *self.sems).start()

        far_first(send)

    def wait(self):
        x, y, up, down, right, left = neighbours()
        others = pl.ds(0, lax.axis_size("gx") * lax.axis_size("gy") - 1)
        remote(self.out.at[others], self.into.at[others], (up, y), *self.sems).wait()


def as_bits(condition):
    return jnp.where(condition, 1.0, 0.0).astype(jnp.bfloat16)


def line_numbers(shape, axis):
    return lax.broadcasted_iota(jnp.int32, shape, axis).astype(jnp.float32)


def dot(a, b, a_dim=1, b_dim=0):
    return lax.dot_general(
        a, b, (((a_dim,), (b_dim,)), ((), ())), preferred_element_type=jnp.float32
    )


def place_blocks(keeper, lines, count):
    i, j = line_numbers((NB, NB), 0), line_numbers((NB, NB), 1)
    owner_row = keeper[...].astype(jnp.float32)
    owner_col = jnp.sum(jnp.where(i == j, owner_row, 0.0), axis=1, keepdims=True)
    same = jnp.where(owner_col == owner_row, 1.0, 0.0)
    rank_row = jnp.sum(jnp.where(i < j, same, 0.0), axis=0, keepdims=True)
    rank_col = jnp.sum(jnp.where(j < i, same, 0.0), axis=1, keepdims=True)
    line_row = lines[...].astype(jnp.float32)
    line_col = jnp.sum(jnp.where(i == j, line_row, 0.0), axis=1, keepdims=True)
    owned = as_bits(line_numbers((count, NB), 0) == owner_row)
    ranked = jnp.where(line_numbers((NB, LANES), 1) == rank_col, line_col + 1.0, 0.0)
    listed = dot(owned, ranked.astype(jnp.bfloat16))
    return owner_row * SLOTS + rank_row, owner_col * SLOTS + rank_col, listed


def regrid(sky, weights, partial, waits):
    slot32 = lax.rem(lax.broadcasted_iota(jnp.int32, (FLUXES * SLOTS, LANES), 0), SLOTS)
    groups = NB // SLOTS
    for g in range(groups):
        if g % (groups // PARTS) == 0:
            waits[g // (groups // PARTS)].wait()
        rows = slice(g * SLOTS, (g + 1) * SLOTS)
        fluxes = sky[:, rows, :].astype(jnp.float32).reshape(FLUXES * SLOTS, OX)
        fluxes = fluxes.astype(jnp.bfloat16)
        total = dot(fluxes, weights[g * SLOTS])
        for n in range(1, SLOTS):
            total = jnp.where(slot32 == n, dot(fluxes, weights[g * SLOTS + n]), total)
        partial[:, rows, :] = total.reshape(FLUXES, SLOTS, LANES)


def fill_send(send, stage, partial, slots, count, most):
    rows = FLUXES * most
    pairs = []
    for f in range(0, FLUXES, 2):
        both = jnp.concatenate([partial[f], partial[f + 1]], axis=1).astype(jnp.bfloat16)
        pairs.append(dot(slots, both))
    for d in range(count):
        for f in range(FLUXES):
            at = d * rows + f * most
            from_lane = (f % 2) * LANES
            stage[at : at + SLOTS] = pairs[f // 2][
                d * SLOTS : (d + 1) * SLOTS, from_lane : from_lane + LANES
            ]
    send[...] = stage[0 : count * rows].reshape(count, rows, LANES).astype(jnp.bfloat16)


def read_targets(listed_in, count):
    lane = line_numbers((SLOTS, LANES), 1)
    row = line_numbers((SLOTS, LANES), 0)
    tiles = []
    for s in range(count):
        line = jnp.broadcast_to(listed_in[s], (SLOTS, LANES))
        line = jnp.sum(jnp.where(lane == row, line, 0.0), axis=1, keepdims=True)
        tiles.append(jnp.where(lane + 1.0 == line, 1.0, 0.0))
    return jnp.concatenate(tiles, axis=0)


def read_fluxes(recv, stage, count, most):
    rows = FLUXES * most
    stage[0 : count * rows] = recv[...].astype(jnp.float32).reshape(count * rows, LANES)
    values = []
    for f in range(FLUXES):
        starts = [s * rows + f * most for s in range(count)]
        tiles = [stage[at : at + SLOTS] for at in starts]
        values.append(jnp.concatenate(tiles, axis=0).astype(jnp.bfloat16))
    return values


def edge_selector(rows, low_row, high_row):
    row = lax.broadcasted_iota(jnp.int32, (rows, BAND_NORTH_COUNT), 0)
    lane = lax.broadcasted_iota(jnp.int32, (rows, BAND_NORTH_COUNT), 1)
    return as_bits(
        ((row == low_row) & (lane == 0)) | ((row == high_row) & (lane == BAND_NORTH_COUNT - 1))
    )


def fill_edges(heat, height, wet, edges):
    selector = edge_selector(8, 0, 1)
    blank = jnp.zeros((EDGES - MARINE_STRATA, LANES), jnp.float32)
    for end in range(4):
        edges[end, MARINE_STRATA:EDGES] = blank
    fields = [heat[k] for k in range(MARINE_STRATA)] + [height, wet]
    for k, values in enumerate(fields):
        row = slice(k, k + 1)
        edges[0, row] = values[0:1]
        edges[1, row] = values[OX - 1 : OX]
        sides = dot(selector, values.astype(jnp.bfloat16), 1, 1)
        edges[2, row] = sides[0:1]
        edges[3, row] = sides[1:2]


class EdgeSwap:
    def __init__(self, edges, got, send_sem, recv_sem):
        self.edges, self.got, self.sems = edges, got, (send_sem, recv_sem)

    def start(self):
        x, y, up, down, right, left = neighbours()
        plan = ((1, 0, (up, y)), (0, 1, (down, y)), (3, 2, (x, right)), (2, 3, (x, left)))
        for src, dst, place in plan:
            remote(self.edges.at[src], self.got.at[dst], place, *self.sems).start()

    def wait(self):
        x, y, up, down, right, left = neighbours()
        remote(self.edges, self.got, (up, y), *self.sems).wait()


def heat_step(heat, got, tall, shore, near, out):
    last = lanes(OX) == LANES - 1
    first = lanes(OX) == 0
    mine = shore[8 : 8 + OX]
    sides = jnp.concatenate([got[3], got[2]], axis=0).astype(jnp.bfloat16)
    wet = dot(sides, edge_selector(2 * EDGES, EDGES + WET_EDGE, WET_EDGE), 0, 0)
    near[0] = jnp.where(last, wet, turn_lanes(mine, -1))
    near[1] = jnp.where(first, wet, turn_lanes(mine, 1))
    for k in range(MARINE_STRATA):
        tall[k, 8 : 8 + OX] = heat[k]
        tall[k, 7:8] = got[0, k : k + 1]
        tall[k, 8 + OX : 9 + OX] = got[1, k : k + 1]
        near[2 + k] = dot(sides, edge_selector(2 * EDGES, EDGES + k, k), 0, 0)

    step = 32
    last, first = last[:step], first[:step]

    def one(k, carry):
        above, below = jnp.maximum(k - 1, 0), jnp.minimum(k + 1, MARINE_STRATA - 1)
        for start in range(0, OX, step):
            rows = slice(start, start + step)
            tall_rows = lambda shift: slice(8 + start + shift, 8 + start + step + shift)
            here = heat[k, rows]
            side = near[2 + k, rows]
            north = jnp.where(last, side, turn_lanes(here, -1))
            south = jnp.where(first, side, turn_lanes(here, 1))
            lateral = shore[tall_rows(1)] * (tall[k, tall_rows(1)] - here)
            lateral = lateral + shore[tall_rows(-1)] * (tall[k, tall_rows(-1)] - here)
            lateral = lateral + near[0, rows] * (north - here)
            lateral = lateral + near[1, rows] * (south - here)
            vertical = (heat[above, rows] - here) + (heat[below, rows] - here)
            out[k, rows] = (here + HORIZ_MIX * lateral + VERT_MIX * vertical) * shore[tall_rows(0)]
        return carry

    lax.fori_loop(0, MARINE_STRATA, one, 0)


class Exchange:
    def __init__(self, rows, edge, packs, sides, send, recv):
        self.rows, self.edge, self.packs, self.sides = rows, edge, packs, sides
        self.sems = [(send.at[k], recv.at[k]) for k in range(3)]

    def start_sides(self):
        x, y, up, down, right, left = neighbours()
        ny = lax.axis_size("gy")
        top, whole, bottom = pl.ds(OX - MARGIN, MARGIN), pl.ds(0, OX), pl.ds(0, MARGIN)
        before, middle, after = pl.ds(0, MARGIN), pl.ds(MARGIN, OX), pl.ds(MARGIN + OX, MARGIN)
        moves = ((top, before, up), (bottom, after, down), (whole, middle, x))

        def send(side, to_y, sems):
            for src, dst, to_x in moves:
                remote(
                    self.packs.at[1 - side, :, src], self.sides.at[side, :, dst], (to_x, to_y), *sems
                ).start()

        pl.when(y < ny - 1)(lambda: send(0, right, self.sems[0]))
        pl.when(y > 0)(lambda: send(1, left, self.sems[1]))

    def start_rows(self):
        x, y, up, down, right, left = neighbours()
        remote(self.rows.at[1], self.edge.at[0], (up, y), *self.sems[2]).start()
        remote(self.rows.at[0], self.edge.at[1], (down, y), *self.sems[2]).start()

    def wait(self):
        x, y, up, down, right, left = neighbours()
        ny = lax.axis_size("gy")
        remote(self.rows, self.edge, (up, y), *self.sems[2]).wait()
        rightward = remote(self.sides.at[0], self.sides.at[0], (up, y), *self.sems[0])
        leftward = remote(self.sides.at[1], self.sides.at[1], (up, y), *self.sems[1])
        pl.when(y > 0)(rightward.wait_recv)
        pl.when(y < ny - 1)(leftward.wait_recv)
        pl.when(y < ny - 1)(rightward.wait_send)
        pl.when(y > 0)(leftward.wait_send)


def clear_walls(sides):
    y, ny = lax.axis_index("gy"), lax.axis_size("gy")
    @pl.when(y == 0)
    def _():
        for side in sides:
            side[0] = jnp.zeros(side.shape[1:], jnp.bfloat16)

    @pl.when(y == ny - 1)
    def _():
        for side in sides:
            side[1] = jnp.zeros(side.shape[1:], jnp.bfloat16)


def fill_rows(rows, field, values):
    rows[0, field] = values[:MARGIN].astype(jnp.bfloat16)
    rows[1, field] = values[OX - MARGIN :].astype(jnp.bfloat16)


def fill_packs(packs, values):
    lane = lanes(OX)
    low = turn_lanes(values[2], LANES - 3 * MARGIN)
    low = jnp.where(lane >= LANES - 2 * MARGIN, turn_lanes(values[1], LANES - 2 * MARGIN), low)
    low = jnp.where(lane >= LANES - MARGIN, turn_lanes(values[0], LANES - MARGIN), low)
    high = turn_lanes(values[2], 3 * MARGIN)
    high = jnp.where(lane < 2 * MARGIN, turn_lanes(values[1], 2 * MARGIN), high)
    high = jnp.where(lane < MARGIN, turn_lanes(values[0], MARGIN), high)
    packs[0, 0] = low.astype(jnp.bfloat16)
    packs[1, 0] = high.astype(jnp.bfloat16)


def fill_packs_from_tiles(packs, state):
    lane = lanes(OX)
    own = slice(BASE, BASE + OX)
    low = turn_lanes(state[2, 0, own], LANES - 4 * MARGIN)
    for f in (1, 0):
        near = lane >= LANES - (f + 1) * MARGIN
        low = jnp.where(near, turn_lanes(state[f, 0, own], LANES - (f + 2) * MARGIN), low)
    shift = LANES - 2 * MARGIN
    high = turn_lanes(state[2, 1, own], 2 * MARGIN - shift)
    for f in (1, 0):
        near = lane < (f + 1) * MARGIN
        high = jnp.where(near, turn_lanes(state[f, 1, own], f * MARGIN - shift), high)
    packs[0, 0] = low.astype(jnp.bfloat16)
    packs[1, 0] = high.astype(jnp.bfloat16)


def zones():
    return (
        (BASE - MARGIN, 0, MARGIN, 0),
        (BASE, MARGIN, OX, None),
        (BASE + OX, MARGIN + OX, MARGIN, 1),
    )


def spread_fields(natural, edge, sides, wide, mask):
    for at, side_at, size, end in zones():
        lane = lanes(size)
        here, there = slice(at, at + size), slice(side_at, side_at + size)
        from_left = sides[0, 0, there].astype(jnp.float32)
        from_right = sides[1, 0, there].astype(jnp.float32)
        for f in range(3):
            centre = natural[f] if end is None else edge[end, f].astype(jnp.float32)
            left = turn_lanes(from_left, -f * MARGIN)
            right = turn_lanes(from_right, f * MARGIN)
            one = jnp.where(lane < MARGIN, left, turn_lanes(centre, MARGIN))
            two = jnp.where(lane >= LANES - MARGIN, right, turn_lanes(centre, -MARGIN))
            if mask is not None and f > 0:
                one = jnp.where(mask[0, here] > 0, one, 0.0)
                two = jnp.where(mask[1, here] > 0, two, 0.0)
            wide[f, 0, here] = one
            wide[f, 1, here] = two


def spread_wet(shore, edge, sides, gain):
    for at, side_at, size, end in zones():
        lane = lanes(size)
        here, there = slice(at, at + size), slice(side_at, side_at + size)
        from_left = sides[0, 1, there].astype(jnp.float32)
        from_right = sides[1, 1, there].astype(jnp.float32)
        centre = shore[8 : 8 + OX] if end is None else edge[end, 3].astype(jnp.float32)
        one = jnp.where(lane >= LANES - MARGIN, from_left, centre)
        two = jnp.where(lane < MARGIN, from_right, centre)
        gain[0, here] = PRESS_GAIN * turn_lanes(one, MARGIN)
        gain[1, here] = PRESS_GAIN * turn_lanes(two, -MARGIN)


def height_over_wall(got, state):
    y, ny = lax.axis_index("gy"), lax.axis_size("gy")
    row = lax.broadcasted_iota(jnp.int32, (2 * EDGES, LANES), 0)
    lane = lanes(2 * EDGES)
    low = (row == EDGES + HEIGHT_EDGE) & (lane == MARGIN - 1)
    high = (row == HEIGHT_EDGE) & (lane == LANES - MARGIN)
    sides = jnp.concatenate([got[3], got[2]], axis=0).astype(jnp.bfloat16)
    values = dot(sides, as_bits(low | high), 0, 0)
    rows, lane = slice(BASE, BASE + OX), lanes(OX)

    @pl.when(y == 0)
    def _():
        state[0, 0, rows] = jnp.where(lane == MARGIN - 1, values, state[0, 0, rows])

    @pl.when(y == ny - 1)
    def _():
        state[0, 1, rows] = jnp.where(lane == LANES - MARGIN, values, state[0, 1, rows])


def renew_overlap(state, reach):
    low, high = BASE - reach, BASE + OX + reach
    shift = LANES - 2 * MARGIN + 2 * OVERLAP
    for start in range(low, high, CHUNK):
        rows = slice(start, start + CHUNK)
        lane = lanes(CHUNK)
        for f in range(3):
            one, two = state[f, 0, rows], state[f, 1, rows]
            state[f, 0, rows] = jnp.where(lane >= LANES - OVERLAP, turn_lanes(two, 2 * MARGIN), one)
            state[f, 1, rows] = jnp.where(lane < OVERLAP, turn_lanes(one, -2 * MARGIN), two)


def own_part(state, f, rows=None):
    one, two = state[f, 0, BASE : BASE + OX], state[f, 1, BASE : BASE + OX]
    return jnp.where(lanes(OX) < HALF, turn_lanes(one, -MARGIN), turn_lanes(two, MARGIN))


def substep(reach, state, forces, gain, turning, raw):
    low, high = BASE - reach, BASE + OX + reach
    turn = [jnp.broadcast_to(turning[tile : tile + 1, :], (CHUNK, LANES)) for tile in range(2)]

    def velocity(start, tile):
        rows = slice(start, start + CHUNK)
        height = state[0, tile, rows]
        slope_east = (
            state[0, tile, start + 1 : start + CHUNK + 1]
            - state[0, tile, start - 1 : start + CHUNK - 1]
        )
        slope_north = turn_lanes(height, -1) - turn_lanes(height, 1)
        old_u, old_v, slope = state[1, tile, rows], state[2, tile, rows], gain[tile, rows]
        new_u = (FLOW_DAMP * old_u + turn[tile] * old_v) + (
            forces[0, tile, rows] - slope * slope_east
        )
        new_v = (FLOW_DAMP * old_v + (forces[1, tile, rows] - slope * slope_north)) - (
            turn[tile] * new_u
        )
        state[1, tile, rows] = new_u
        state[2, tile, rows] = new_v

    def surface(start, tile):
        rows = slice(start, start + CHUNK)
        flow_north = state[2, tile, rows]
        spread_east = (
            state[1, tile, start + 1 : start + CHUNK + 1]
            - state[1, tile, start - 1 : start + CHUNK - 1]
        )
        spread_north = turn_lanes(flow_north, -1) - turn_lanes(flow_north, 1)
        height, slope = state[0, tile, rows], gain[tile, rows]
        if raw:
            height = jnp.where(slope > 0, height, 0.0)
        state[0, tile, rows] = (height - forces[2, tile, rows]) - slope * (
            spread_east + spread_north
        )

    starts = range(low, high, CHUNK)
    for start in starts:
        for tile in range(2):
            velocity(start, tile)
    for start in starts:
        for tile in range(2):
            surface(start, tile)


def run_span(state, forces, gain, turning, raw):
    done = 0
    while done < SPAN:
        need = 2 * (SPAN - done) - 1
        reach = -(-need // 8) * 8
        steps = min(SPAN - done, GROUP)
        if done == RENEW:
            renew_overlap(state, reach)
        if raw and done == 0:
            substep(reach, state, forces, gain, turning, True)

        def one(_, carry, reach=reach):
            substep(reach, state, forces, gain, turning, False)
            return carry

        lax.fori_loop(1 if raw and done == 0 else 0, steps, one, 0, unroll=True)
        done += steps


def window_kernel(
    sky_far, weights_far, keeper_far, lines_far, sea_far, heat_far, h_far, u_far, v_far,
    back, heat_out, out,
    sky, weights, keeper, lines, sea, heat, natural,
    turning, partial, stage, send, recv, listed_out, listed_in, skin_send, skin_recv,
    heat_edges, heat_got, tall, near, shore,
    state, forces, gain,
    rows1, edge1, packs1, sides1,
    rows2, edge2, packs2, sides2, rows3, edge3, packs3, sides3,
    load_sem, list_send, list_recv, a2a_send, a2a_recv, skin_send_sem, skin_recv_sem,
    heat_send_sem, heat_recv_sem, send1, recv1, send2, recv2, send3, recv3,
):
    ny = lax.axis_size("gy")
    count = lax.axis_size("gx") * ny
    most = max(2, 2 * NB // count)
    me = lax.axis_index("gx") * ny + lax.axis_index("gy")
    part = NB // PARTS
    pieces = [pl.ds(p * part, part) for p in range(PARTS)]
    moves = [(keeper_far, keeper), (lines_far, lines), (sky_far, sky)]
    moves += [(weights_far.at[pieces[0]], weights.at[pieces[0]])]
    moves += [(sea_far, sea), (h_far, natural.at[0]), (heat_far, heat)]
    moves += [(weights_far.at[piece], weights.at[piece]) for piece in pieces[1:]]
    moves += [(u_far, natural.at[1]), (v_far, natural.at[2])]
    loads = [
        pltpu.make_async_copy(src, dst, load_sem.at[k]) for k, (src, dst) in enumerate(moves)
    ]
    for load in loads:
        load.start()
    greet_all()
    turning[...] = turning_rows()
    clear_walls((sides1, sides2, sides3))
    blank = jnp.zeros((8, LANES), jnp.float32)
    for f in range(2):
        for tile in range(2):
            state[f, tile, BASE - MARGIN - 8 : BASE - MARGIN] = blank
            state[f, tile, BASE + OX + MARGIN : BASE + OX + MARGIN + 8] = blank
    stage[count * FLUXES * most : count * FLUXES * most + SLOTS] = blank
    loads[0].wait()
    loads[1].wait()
    key_row, key_col, listed = place_blocks(keeper, lines, count)
    for d in range(count):
        listed_out[d] = listed[d : d + 1]
    slots = as_bits(line_numbers((count * SLOTS, NB), 0) == key_row)
    for load in loads[4:7]:
        load.wait()
    lat = lax.axis_index("gy") * LANES + lanes(OX)
    inside = (lat > 0) & (lat < ny * LANES - 1)
    shore[8 : 8 + OX] = jnp.where(inside, sea[...].astype(jnp.float32), 0.0)
    fill_edges(heat, natural[0], shore[8 : 8 + OX], heat_edges)
    heats = EdgeSwap(heat_edges, heat_got, heat_send_sem, heat_recv_sem)
    targets = Swap(listed_out, listed_in, list_send, list_recv)
    fluxes = Swap(send, recv, a2a_send, a2a_recv)
    skins = Swap(skin_send, skin_recv, skin_send_sem, skin_recv_sem)
    loads[2].wait()
    regrid(sky, weights, partial, [loads[3]] + loads[7 : 6 + PARTS])
    fill_send(send, stage, partial, slots, count, most)
    pl.semaphore_wait(pltpu.get_barrier_semaphore(), count - 1)
    heats.start()
    targets.start()
    fluxes.start()
    recv[me] = send[me]
    listed_in[me] = listed_out[me]
    for load in loads[6 + PARTS :]:
        load.wait()
    fill_packs(packs1, [natural[f] for f in range(3)])
    for side in range(2):
        packs1[side, 1] = shore[8 : 8 + OX].astype(jnp.bfloat16)
    for f in range(3):
        fill_rows(rows1, f, natural[f])
    fill_rows(rows1, 3, shore[8 : 8 + OX])
    first = Exchange(rows1, edge1, packs1, sides1, send1, recv1)
    first.start_sides()
    first.start_rows()
    heats.wait()
    shore[7:8] = heat_got[0, WET_EDGE : WET_EDGE + 1]
    shore[8 + OX : 9 + OX] = heat_got[1, WET_EDGE : WET_EDGE + 1]
    heat_step(heat, heat_got, tall, shore, near, heat_out)
    targets.wait()
    target = read_targets(listed_in, count)
    target_turned = target.T.astype(jnp.bfloat16)
    target = target.astype(jnp.bfloat16)
    fluxes.wait()
    values = read_fluxes(recv, stage, count, most)
    stress = dot(target_turned, jnp.concatenate([values[0], values[1]], axis=1))
    others = dot(target_turned, jnp.concatenate([values[3], values[2]], axis=1))
    mask = shore[8 : 8 + OX]
    own = [
        WIND_GAIN * stress[:, :LANES] * mask,
        WIND_GAIN * stress[:, LANES:] * mask,
        FRESH_GAIN * others[:, :LANES] * mask,
    ]
    second = Exchange(rows2, edge2, packs2, sides2, send2, recv2)
    fill_packs(packs2, own)
    second.start_sides()
    for f in range(3):
        fill_rows(rows2, f, own[f])
    second.start_rows()
    first.wait()
    spread_wet(shore, edge1, sides1, gain)
    spread_fields(natural, edge1, sides1, state, gain)
    height_over_wall(heat_got, state)
    surface = heat_out[0] + HEAT_GAIN * others[:, LANES:] * shore[8 : 8 + OX]
    heat_out[0] = surface
    band = dot(target, surface.astype(jnp.bfloat16))
    skin_send[...] = band.reshape(count, SLOTS, LANES).astype(jnp.bfloat16)
    skins.start()
    skin_recv[me] = skin_send[me]
    second.wait()
    spread_fields(own, edge2, sides2, forces, None)
    run_span(state, forces, gain, turning, True)
    third = Exchange(rows3, edge3, packs3, sides3, send3, recv3)
    fill_packs_from_tiles(packs3, state)
    third.start_sides()
    for f in range(3):
        natural[f] = own_part(state, f)
        fill_rows(rows3, f, natural[f])
    third.start_rows()
    skins.wait()
    slots = as_bits(line_numbers((NB, count * SLOTS), 1) == key_col)
    skin = dot(slots, skin_recv[...].reshape(count * SLOTS, LANES))
    slot8 = lax.broadcasted_iota(jnp.int32, (SLOTS, LANES), 0)
    for g in range(NB // SLOTS):
        rows = slice(g * SLOTS, (g + 1) * SLOTS)
        lines_skin = skin[rows].astype(jnp.bfloat16)
        total = dot(lines_skin, weights[g * SLOTS], 1, 1)
        for n in range(1, SLOTS):
            total = jnp.where(slot8 == n, dot(lines_skin, weights[g * SLOTS + n], 1, 1), total)
        back[rows] = total
    third.wait()
    spread_fields(natural, edge3, sides3, state, None)
    run_span(state, forces, gain, turning, False)
    for f in range(3):
        out[f] = own_part(state, f)


def turning_rows():
    total_y = lax.axis_size("gy") * LANES
    shape = (8, LANES)
    lane = lax.broadcasted_iota(jnp.int32, shape, 1)
    tile = lax.broadcasted_iota(jnp.int32, shape, 0)
    rows = lax.axis_index("gy") * LANES + lane + jnp.where(tile == 0, -MARGIN, MARGIN)
    rows = jnp.where(rows < 0, rows + total_y, jnp.where(rows < total_y, rows, rows - total_y))
    return CORIOLIS * jnp.sin(jnp.pi * ((rows.astype(jnp.float32) + 0.5) / total_y - 0.5))


def hand_over(*refs):
    sources, targets, stores = refs[:3], refs[3:6], refs[6]
    away = [pltpu.make_async_copy(sources[k], targets[k], stores.at[k]) for k in range(3)]
    for copy in away:
        copy.start()
    for copy in away:
        copy.wait()


def per_device(
    sky_interface_transfers,
    coupling_matrix_enlarged,
    piece_keeper_part,
    receiving_part_line,
    marine_point_switch,
    potential_heat_deviation,
    free_marine_lift,
    depth_averaged_uflow,
    depth_averaged_vflow,
):
    count = lax.axis_size("gx") * lax.axis_size("gy")
    most = max(2, 2 * NB // count)
    line = LANES
    half = jnp.bfloat16
    full = jnp.float32

    def boxes(fields, kinds):
        return [
            pltpu.VMEM((2, fields, MARGIN, line), half),
            pltpu.VMEM((2, fields, MARGIN, line), half),
            pltpu.VMEM((2, kinds, OX, line), half),
            pltpu.VMEM((2, kinds, FRAME, line), half),
        ]

    inside = pl.BlockSpec(memory_space=pltpu.VMEM)
    far = pl.BlockSpec(memory_space=pltpu.HBM)
    shapes = (
        jax.ShapeDtypeStruct((NB, OX), full),
        jax.ShapeDtypeStruct((MARINE_STRATA, OX, line), full),
        jax.ShapeDtypeStruct((3, OX, line), full),
    )
    results = pl.pallas_call(
        window_kernel,
        out_shape=shapes,
        in_specs=[far] * 9,
        out_specs=(inside,) * 3,
        scratch_shapes=[
            pltpu.VMEM((FLUXES, NB, OX), half),
            pltpu.VMEM((NB, OX, line), half),
            pltpu.VMEM((1, NB), jnp.int32),
            pltpu.VMEM((1, NB), jnp.int32),
            pltpu.VMEM((OX, line), jnp.int32),
            pltpu.VMEM((MARINE_STRATA, OX, line), full),
            pltpu.VMEM((3, OX, line), full),
            pltpu.VMEM((8, line), full),
            pltpu.VMEM((FLUXES, NB, line), full),
            pltpu.VMEM((count * FLUXES * most + SLOTS, line), full),
            pltpu.VMEM((count, FLUXES * most, line), half),
            pltpu.VMEM((count, FLUXES * most, line), half),
            pltpu.VMEM((count, 1, line), full),
            pltpu.VMEM((count, 1, line), full),
            pltpu.VMEM((count, SLOTS, line), half),
            pltpu.VMEM((count, SLOTS, line), half),
            pltpu.VMEM((4, EDGES, line), full),
            pltpu.VMEM((4, EDGES, line), full),
            pltpu.VMEM((MARINE_STRATA, OX + 16, line), full),
            pltpu.VMEM((2 + MARINE_STRATA, OX, line), full),
            pltpu.VMEM((OX + 16, line), full),
            pltpu.VMEM((3, 2, TALL, line), full),
            pltpu.VMEM((3, 2, TALL, line), full),
            pltpu.VMEM((2, TALL, line), full),
        ]
        + boxes(4, 2)
        + boxes(3, 1)
        + boxes(3, 1)
        + [pltpu.SemaphoreType.DMA((3 + PARTS + 5,))]
        + [pltpu.SemaphoreType.DMA] * 8
        + [pltpu.SemaphoreType.DMA((3,))] * 6,
        compiler_params=pltpu.CompilerParams(
            collective_id=0, has_side_effects=True, vmem_limit_bytes=24 * 1024 * 1024
        ),
        name="window",
    )(
        *[
            pltpu.with_memory_space_constraint(value, pltpu.HBM)
            for value in (
                sky_interface_transfers,
                coupling_matrix_enlarged,
                piece_keeper_part.reshape(1, NB),
                receiving_part_line,
                marine_point_switch,
                potential_heat_deviation,
                free_marine_lift,
                depth_averaged_uflow,
                depth_averaged_vflow,
            )
        ]
    )
    anywhere = pl.BlockSpec(memory_space=pl.ANY)
    return pl.pallas_call(
        hand_over,
        out_shape=shapes,
        in_specs=[anywhere] * 3,
        out_specs=(anywhere,) * 3,
        scratch_shapes=[pltpu.SemaphoreType.DMA((3,))],
        compiler_params=pltpu.CompilerParams(vmem_limit_bytes=8 * 1024 * 1024),
        name="hand_over",
    )(*results)


def solution(mesh):
    in_specs = (
        P(None, "gy", "gx"),
        P("gy", "gx", None),
        P("gx", "gy", None),
        P("gx", "gy"),
        P("gx", "gy"),
        P(None, "gx", "gy"),
        P("gx", "gy"),
        P("gx", "gy"),
        P("gx", "gy"),
    )
    out_specs = (P("gy", "gx"), P(None, "gx", "gy"), P(None, "gx", "gy"))
    return jax.shard_map(
        per_device, mesh=mesh, in_specs=in_specs, out_specs=out_specs, check_vma=False
    )
```

```python
import jax
import jax.numpy as jnp
from jax import lax
from jax.experimental import pallas as pl
from jax.experimental.pallas import tpu as pltpu
from jax.sharding import PartitionSpec as P

NB = 96
OX = 128
BAND_NORTH_COUNT = 128
MARINE_STRATA = 8
SUB = 40


HORIZ_MIX = 0.15
VERT_MIX = 0.2
HEAT_GAIN = 0.5
FLOW_DAMP = 0.98
PRESS_GAIN = 0.6
DIVERGE_GAIN = 0.6
CORIOLIS = 0.1
WIND_GAIN = 0.05
FRESH_GAIN = 0.05


MESH = pl.DeviceIdType.MESH
LANES = BAND_NORTH_COUNT
HALF = LANES // 2
SPAN = SUB // 2
MARGIN = 2 * SPAN
BASE = MARGIN + 8
TALL = OX + 2 * BASE
FRAME = OX + 2 * MARGIN
OVERLAP = (LANES - 2 * MARGIN) // 2
GROUP = 4
RENEW = 3 * GROUP
CHUNK = 16
SLOTS = 8
FLUXES = 4
URGENT = 3
PARTS = 4
EDGES = 16
HEIGHT_EDGE = MARINE_STRATA
WET_EDGE = MARINE_STRATA + 1


def turn_lanes(values, shift):
    shift = shift % LANES
    return pltpu.roll(values, shift, 1) if shift else values


def lanes(rows):
    return lax.broadcasted_iota(jnp.int32, (rows, LANES), 1)


def neighbours():
    nx, ny = lax.axis_size("gx"), lax.axis_size("gy")
    x, y = lax.axis_index("gx"), lax.axis_index("gy")
    up, down = lax.rem(x + 1, nx), lax.rem(x + nx - 1, nx)
    right, left = lax.rem(y + 1, ny), lax.rem(y + ny - 1, ny)
    return x, y, up, down, right, left


def far_first(act):
    nx, ny = lax.axis_size("gx"), lax.axis_size("gy")
    x, y = lax.axis_index("gx"), lax.axis_index("gy")
    for dy in sorted(range(ny), key=lambda d: abs(2 * d - ny)):

        def one(dx, carry, dy=dy):
            act(lax.rem(x + dx, nx), lax.rem(y + dy, ny))
            return carry

        lax.fori_loop(0 if dy else 1, nx, one, 0, unroll=True)


def greet_all():
    barrier = pltpu.get_barrier_semaphore()

    def greet(to_x, to_y):
        pl.semaphore_signal(barrier, inc=1, device_id=(to_x, to_y), device_id_type=MESH)

    far_first(greet)


def remote(src, dst, place, send_sem, recv_sem):
    return pltpu.make_async_remote_copy(
        src_ref=src,
        dst_ref=dst,
        send_sem=send_sem,
        recv_sem=recv_sem,
        device_id=place,
        device_id_type=MESH,
    )


class Swap:
    def __init__(self, out, into, send_sem, recv_sem, rows):
        self.out, self.into, self.sems = out, into, (send_sem, recv_sem)
        self.rows = pl.ds(0, rows)

    def start(self):
        ny = lax.axis_size("gy")
        me = lax.axis_index("gx") * ny + lax.axis_index("gy")

        def send(to_x, to_y):
            place = (to_x, to_y)
            src, dst = self.out.at[to_x * ny + to_y, self.rows], self.into.at[me, self.rows]
            remote(src, dst, place, *self.sems).start()

        far_first(send)

    def wait(self):
        x, y, up, down, right, left = neighbours()
        others = pl.ds(0, lax.axis_size("gx") * lax.axis_size("gy") - 1)
        src, dst = self.out.at[others, self.rows], self.into.at[others, self.rows]
        remote(src, dst, (up, y), *self.sems).wait()


def as_bits(condition):
    return jnp.where(condition, 1.0, 0.0).astype(jnp.bfloat16)


def line_numbers(shape, axis):
    return lax.broadcasted_iota(jnp.int32, shape, axis).astype(jnp.float32)


def dot(a, b, a_dim=1, b_dim=0):
    return lax.dot_general(
        a, b, (((a_dim,), (b_dim,)), ((), ())), preferred_element_type=jnp.float32
    )


def place_blocks(keeper, lines, count):
    i, j = line_numbers((NB, NB), 0), line_numbers((NB, NB), 1)
    owner_row = keeper[...].astype(jnp.float32)
    owner_col = jnp.sum(jnp.where(i == j, owner_row, 0.0), axis=1, keepdims=True)
    same = jnp.where(owner_col == owner_row, 1.0, 0.0)
    rank_row = jnp.sum(jnp.where(i < j, same, 0.0), axis=0, keepdims=True)
    rank_col = jnp.sum(jnp.where(j < i, same, 0.0), axis=1, keepdims=True)
    line_row = lines[...].astype(jnp.float32)
    line_col = jnp.sum(jnp.where(i == j, line_row, 0.0), axis=1, keepdims=True)
    owned = as_bits(line_numbers((count, NB), 0) == owner_row)
    ranked = jnp.where(line_numbers((NB, LANES), 1) == rank_col, line_col + 1.0, 0.0)
    listed = dot(owned, ranked.astype(jnp.bfloat16))
    return owner_row * SLOTS + rank_row, owner_col * SLOTS + rank_col, listed


def regrid(sky, weights, partial, waits):
    slot32 = lax.rem(lax.broadcasted_iota(jnp.int32, (FLUXES * SLOTS, LANES), 0), SLOTS)
    groups = NB // SLOTS
    for g in range(groups):
        if g % (groups // PARTS) == 0:
            waits[g // (groups // PARTS)].wait()
        rows = slice(g * SLOTS, (g + 1) * SLOTS)
        fluxes = sky[:, rows, :].astype(jnp.float32).reshape(FLUXES * SLOTS, OX)
        fluxes = fluxes.astype(jnp.bfloat16)
        total = dot(fluxes, weights[g * SLOTS])
        for n in range(1, SLOTS):
            total = jnp.where(slot32 == n, dot(fluxes, weights[g * SLOTS + n]), total)
        partial[:, rows, :] = total.reshape(FLUXES, SLOTS, LANES)


def fill_send(send, heat_send, stage, partial, slots, count, most):
    rows = FLUXES * most
    pairs = []
    for f, g in ((0, 1), (3, 2)):
        both = jnp.concatenate([partial[f], partial[g]], axis=1).astype(jnp.bfloat16)
        pairs.append(dot(slots, both))
    sources = [pairs[0][:, :LANES], pairs[0][:, LANES:], pairs[1][:, :LANES]]
    for d in range(count):
        for k, source in enumerate(sources):
            at = d * rows + k * most
            stage[at : at + SLOTS] = source[d * SLOTS : (d + 1) * SLOTS]
    send[...] = stage[0 : count * rows].reshape(count, rows, LANES).astype(jnp.bfloat16)
    heat_send[...] = pairs[1][:, LANES:].reshape(count, SLOTS, LANES).astype(jnp.bfloat16)


def read_targets(listed_in, count):
    lane = line_numbers((SLOTS, LANES), 1)
    row = line_numbers((SLOTS, LANES), 0)
    tiles = []
    for s in range(count):
        line = jnp.broadcast_to(listed_in[s], (SLOTS, LANES))
        line = jnp.sum(jnp.where(lane == row, line, 0.0), axis=1, keepdims=True)
        tiles.append(jnp.where(lane + 1.0 == line, 1.0, 0.0))
    return jnp.concatenate(tiles, axis=0)


def received(values, rows):
    row = lax.broadcasted_iota(jnp.int32, values.shape, 1)
    flat = (values.shape[0] * values.shape[1], LANES)
    return jnp.where(row < rows, values.astype(jnp.float32), 0.0).reshape(flat)


def read_fluxes(recv, stage, count, most):
    rows = FLUXES * most
    stage[0 : count * rows] = received(recv[...], URGENT * most)
    values = []
    for k in range(URGENT):
        starts = [s * rows + k * most for s in range(count)]
        tiles = [stage[at : at + SLOTS] for at in starts]
        values.append(jnp.concatenate(tiles, axis=0).astype(jnp.bfloat16))
    return values


def edge_selector(rows, low_row, high_row):
    row = lax.broadcasted_iota(jnp.int32, (rows, BAND_NORTH_COUNT), 0)
    lane = lax.broadcasted_iota(jnp.int32, (rows, BAND_NORTH_COUNT), 1)
    return as_bits(
        ((row == low_row) & (lane == 0)) | ((row == high_row) & (lane == BAND_NORTH_COUNT - 1))
    )


def fill_edges(heat, height, wet, edges):
    selector = edge_selector(8, 0, 1)
    blank = jnp.zeros((EDGES - MARINE_STRATA, LANES), jnp.float32)
    for end in range(4):
        edges[end, MARINE_STRATA:EDGES] = blank
    fields = [heat[k] for k in range(MARINE_STRATA)] + [height, wet]
    for k, values in enumerate(fields):
        row = slice(k, k + 1)
        edges[0, row] = values[0:1]
        edges[1, row] = values[OX - 1 : OX]
        sides = dot(selector, values.astype(jnp.bfloat16), 1, 1)
        edges[2, row] = sides[0:1]
        edges[3, row] = sides[1:2]


class EdgeSwap:
    def __init__(self, edges, got, send_sem, recv_sem):
        self.edges, self.got, self.sems = edges, got, (send_sem, recv_sem)

    def start(self):
        x, y, up, down, right, left = neighbours()
        plan = ((1, 0, (up, y)), (0, 1, (down, y)), (3, 2, (x, right)), (2, 3, (x, left)))
        for src, dst, place in plan:
            remote(self.edges.at[src], self.got.at[dst], place, *self.sems).start()

    def wait(self):
        x, y, up, down, right, left = neighbours()
        remote(self.edges, self.got, (up, y), *self.sems).wait()


def heat_step(heat, got, tall, shore, near, out):
    last = lanes(OX) == LANES - 1
    first = lanes(OX) == 0
    mine = shore[8 : 8 + OX]
    sides = jnp.concatenate([got[3], got[2]], axis=0).astype(jnp.bfloat16)
    wet = dot(sides, edge_selector(2 * EDGES, EDGES + WET_EDGE, WET_EDGE), 0, 0)
    near[0] = jnp.where(last, wet, turn_lanes(mine, -1))
    near[1] = jnp.where(first, wet, turn_lanes(mine, 1))
    for k in range(MARINE_STRATA):
        tall[k, 8 : 8 + OX] = heat[k]
        tall[k, 7:8] = got[0, k : k + 1]
        tall[k, 8 + OX : 9 + OX] = got[1, k : k + 1]
        near[2 + k] = dot(sides, edge_selector(2 * EDGES, EDGES + k, k), 0, 0)

    step = 32
    last, first = last[:step], first[:step]

    def one(k, carry):
        above, below = jnp.maximum(k - 1, 0), jnp.minimum(k + 1, MARINE_STRATA - 1)
        for start in range(0, OX, step):
            rows = slice(start, start + step)
            tall_rows = lambda shift: slice(8 + start + shift, 8 + start + step + shift)
            here = heat[k, rows]
            side = near[2 + k, rows]
            north = jnp.where(last, side, turn_lanes(here, -1))
            south = jnp.where(first, side, turn_lanes(here, 1))
            lateral = shore[tall_rows(1)] * (tall[k, tall_rows(1)] - here)
            lateral = lateral + shore[tall_rows(-1)] * (tall[k, tall_rows(-1)] - here)
            lateral = lateral + near[0, rows] * (north - here)
            lateral = lateral + near[1, rows] * (south - here)
            vertical = (heat[above, rows] - here) + (heat[below, rows] - here)
            out[k, rows] = (here + HORIZ_MIX * lateral + VERT_MIX * vertical) * shore[tall_rows(0)]
        return carry

    lax.fori_loop(0, MARINE_STRATA, one, 0)


class Exchange:
    def __init__(self, rows, edge, packs, sides, send, recv):
        self.rows, self.edge, self.packs, self.sides = rows, edge, packs, sides
        self.sems = [(send.at[k], recv.at[k]) for k in range(3)]

    def start_sides(self):
        x, y, up, down, right, left = neighbours()
        ny = lax.axis_size("gy")
        top, whole, bottom = pl.ds(OX - MARGIN, MARGIN), pl.ds(0, OX), pl.ds(0, MARGIN)
        before, middle, after = pl.ds(0, MARGIN), pl.ds(MARGIN, OX), pl.ds(MARGIN + OX, MARGIN)
        moves = ((top, before, up), (bottom, after, down), (whole, middle, x))

        def send(side, to_y, sems):
            for src, dst, to_x in moves:
                remote(
                    self.packs.at[1 - side, :, src], self.sides.at[side, :, dst], (to_x, to_y), *sems
                ).start()

        pl.when(y < ny - 1)(lambda: send(0, right, self.sems[0]))
        pl.when(y > 0)(lambda: send(1, left, self.sems[1]))

    def start_rows(self):
        x, y, up, down, right, left = neighbours()
        remote(self.rows.at[1], self.edge.at[0], (up, y), *self.sems[2]).start()
        remote(self.rows.at[0], self.edge.at[1], (down, y), *self.sems[2]).start()

    def wait(self):
        x, y, up, down, right, left = neighbours()
        ny = lax.axis_size("gy")
        remote(self.rows, self.edge, (up, y), *self.sems[2]).wait()
        rightward = remote(self.sides.at[0], self.sides.at[0], (up, y), *self.sems[0])
        leftward = remote(self.sides.at[1], self.sides.at[1], (up, y), *self.sems[1])
        pl.when(y > 0)(rightward.wait_recv)
        pl.when(y < ny - 1)(leftward.wait_recv)
        pl.when(y < ny - 1)(rightward.wait_send)
        pl.when(y > 0)(leftward.wait_send)


def clear_walls(sides):
    y, ny = lax.axis_index("gy"), lax.axis_size("gy")
    @pl.when(y == 0)
    def _():
        for side in sides:
            side[0] = jnp.zeros(side.shape[1:], jnp.bfloat16)

    @pl.when(y == ny - 1)
    def _():
        for side in sides:
            side[1] = jnp.zeros(side.shape[1:], jnp.bfloat16)


def fill_rows(rows, field, values):
    rows[0, field] = values[:MARGIN].astype(jnp.bfloat16)
    rows[1, field] = values[OX - MARGIN :].astype(jnp.bfloat16)


def fill_packs(packs, values):
    lane = lanes(OX)
    low = turn_lanes(values[2], LANES - 3 * MARGIN)
    low = jnp.where(lane >= LANES - 2 * MARGIN, turn_lanes(values[1], LANES - 2 * MARGIN), low)
    low = jnp.where(lane >= LANES - MARGIN, turn_lanes(values[0], LANES - MARGIN), low)
    high = turn_lanes(values[2], 3 * MARGIN)
    high = jnp.where(lane < 2 * MARGIN, turn_lanes(values[1], 2 * MARGIN), high)
    high = jnp.where(lane < MARGIN, turn_lanes(values[0], MARGIN), high)
    packs[0, 0] = low.astype(jnp.bfloat16)
    packs[1, 0] = high.astype(jnp.bfloat16)


def fill_packs_from_tiles(packs, state):
    lane = lanes(OX)
    own = slice(BASE, BASE + OX)
    low = turn_lanes(state[2, 0, own], LANES - 4 * MARGIN)
    for f in (1, 0):
        near = lane >= LANES - (f + 1) * MARGIN
        low = jnp.where(near, turn_lanes(state[f, 0, own], LANES - (f + 2) * MARGIN), low)
    shift = LANES - 2 * MARGIN
    high = turn_lanes(state[2, 1, own], 2 * MARGIN - shift)
    for f in (1, 0):
        near = lane < (f + 1) * MARGIN
        high = jnp.where(near, turn_lanes(state[f, 1, own], f * MARGIN - shift), high)
    packs[0, 0] = low.astype(jnp.bfloat16)
    packs[1, 0] = high.astype(jnp.bfloat16)


def fill_rows_from_tiles(rows, field, state):
    for end, start in enumerate((BASE, BASE + OX - MARGIN)):
        here = slice(start, start + MARGIN)
        one = turn_lanes(state[field, 0, here], -MARGIN)
        two = turn_lanes(state[field, 1, here], MARGIN)
        rows[end, field] = jnp.where(lanes(MARGIN) < HALF, one, two).astype(jnp.bfloat16)


def zones():
    return (
        (BASE - MARGIN, 0, MARGIN, 0),
        (BASE, MARGIN, OX, None),
        (BASE + OX, MARGIN + OX, MARGIN, 1),
    )


def place_own(natural, wide):
    here = slice(BASE, BASE + OX)
    for f in range(3):
        wide[f, 0, here] = turn_lanes(natural[f], MARGIN)
        wide[f, 1, here] = turn_lanes(natural[f], -MARGIN)


def spread_fields(edge, sides, wide, mask):
    for at, side_at, size, end in zones():
        lane = lanes(size)
        here, there = slice(at, at + size), slice(side_at, side_at + size)
        from_left = sides[0, 0, there].astype(jnp.float32)
        from_right = sides[1, 0, there].astype(jnp.float32)
        for f in range(3):
            if end is None:
                one, two = wide[f, 0, here], wide[f, 1, here]
            else:
                centre = edge[end, f].astype(jnp.float32)
                one, two = turn_lanes(centre, MARGIN), turn_lanes(centre, -MARGIN)
            one = jnp.where(lane < MARGIN, turn_lanes(from_left, -f * MARGIN), one)
            two = jnp.where(lane >= LANES - MARGIN, turn_lanes(from_right, f * MARGIN), two)
            if mask is not None and f > 0:
                one = jnp.where(mask[0, here] > 0, one, 0.0)
                two = jnp.where(mask[1, here] > 0, two, 0.0)
            wide[f, 0, here] = one
            wide[f, 1, here] = two


def spread_wet(shore, edge, sides, gain):
    for at, side_at, size, end in zones():
        lane = lanes(size)
        here, there = slice(at, at + size), slice(side_at, side_at + size)
        from_left = sides[0, 1, there].astype(jnp.float32)
        from_right = sides[1, 1, there].astype(jnp.float32)
        centre = shore[8 : 8 + OX] if end is None else edge[end, 3].astype(jnp.float32)
        one = jnp.where(lane >= LANES - MARGIN, from_left, centre)
        two = jnp.where(lane < MARGIN, from_right, centre)
        gain[0, here] = PRESS_GAIN * turn_lanes(one, MARGIN)
        gain[1, here] = PRESS_GAIN * turn_lanes(two, -MARGIN)


def height_over_wall(got, state):
    y, ny = lax.axis_index("gy"), lax.axis_size("gy")
    row = lax.broadcasted_iota(jnp.int32, (2 * EDGES, LANES), 0)
    lane = lanes(2 * EDGES)
    low = (row == EDGES + HEIGHT_EDGE) & (lane == MARGIN - 1)
    high = (row == HEIGHT_EDGE) & (lane == LANES - MARGIN)
    sides = jnp.concatenate([got[3], got[2]], axis=0).astype(jnp.bfloat16)
    values = dot(sides, as_bits(low | high), 0, 0)
    rows, lane = slice(BASE, BASE + OX), lanes(OX)

    @pl.when(y == 0)
    def _():
        state[0, 0, rows] = jnp.where(lane == MARGIN - 1, values, state[0, 0, rows])

    @pl.when(y == ny - 1)
    def _():
        state[0, 1, rows] = jnp.where(lane == LANES - MARGIN, values, state[0, 1, rows])


def renew_overlap(state, reach):
    low, high = BASE - reach, BASE + OX + reach
    shift = LANES - 2 * MARGIN + 2 * OVERLAP
    for start in range(low, high, CHUNK):
        rows = slice(start, start + CHUNK)
        lane = lanes(CHUNK)
        for f in range(3):
            one, two = state[f, 0, rows], state[f, 1, rows]
            state[f, 0, rows] = jnp.where(lane >= LANES - OVERLAP, turn_lanes(two, 2 * MARGIN), one)
            state[f, 1, rows] = jnp.where(lane < OVERLAP, turn_lanes(one, -2 * MARGIN), two)


def own_part(state, f, rows=None):
    one, two = state[f, 0, BASE : BASE + OX], state[f, 1, BASE : BASE + OX]
    return jnp.where(lanes(OX) < HALF, turn_lanes(one, -MARGIN), turn_lanes(two, MARGIN))


def substep(reach, state, forces, gain, turning, raw):
    low, high = BASE - reach, BASE + OX + reach
    turn = [jnp.broadcast_to(turning[tile : tile + 1, :], (CHUNK, LANES)) for tile in range(2)]

    def velocity(start, tile):
        rows = slice(start, start + CHUNK)
        height = state[0, tile, rows]
        slope_east = (
            state[0, tile, start + 1 : start + CHUNK + 1]
            - state[0, tile, start - 1 : start + CHUNK - 1]
        )
        slope_north = turn_lanes(height, -1) - turn_lanes(height, 1)
        old_u, old_v, slope = state[1, tile, rows], state[2, tile, rows], gain[tile, rows]
        new_u = (FLOW_DAMP * old_u + turn[tile] * old_v) + (
            forces[0, tile, rows] - slope * slope_east
        )
        new_v = (FLOW_DAMP * old_v + (forces[1, tile, rows] - slope * slope_north)) - (
            turn[tile] * new_u
        )
        state[1, tile, rows] = new_u
        state[2, tile, rows] = new_v

    def surface(start, tile):
        rows = slice(start, start + CHUNK)
        flow_north = state[2, tile, rows]
        spread_east = (
            state[1, tile, start + 1 : start + CHUNK + 1]
            - state[1, tile, start - 1 : start + CHUNK - 1]
        )
        spread_north = turn_lanes(flow_north, -1) - turn_lanes(flow_north, 1)
        height, slope = state[0, tile, rows], gain[tile, rows]
        if raw:
            height = jnp.where(slope > 0, height, 0.0)
        state[0, tile, rows] = (height - forces[2, tile, rows]) - slope * (
            spread_east + spread_north
        )

    starts = range(low, high, CHUNK)
    for start in starts:
        for tile in range(2):
            velocity(start, tile)
    for start in starts:
        for tile in range(2):
            surface(start, tile)


def run_span(state, forces, gain, turning, raw):
    done = 0
    while done < SPAN:
        need = 2 * (SPAN - done) - 1
        reach = -(-need // 8) * 8
        steps = min(SPAN - done, GROUP)
        if done == RENEW:
            renew_overlap(state, reach)
        if raw and done == 0:
            substep(reach, state, forces, gain, turning, True)

        def one(_, carry, reach=reach):
            substep(reach, state, forces, gain, turning, False)
            return carry

        lax.fori_loop(1 if raw and done == 0 else 0, steps, one, 0, unroll=True)
        done += steps


def window_kernel(
    sky_far, weights_far, keeper_far, lines_far, sea_far, heat_far, h_far, u_far, v_far,
    back, heat_out, out,
    sky, weights, keeper, lines, sea, heat, natural,
    turning, partial, stage, send, recv, warm_send, warm_recv, listed_out, listed_in, skin_send, skin_recv,
    heat_edges, heat_got, tall, near, shore,
    state, forces, gain,
    rows1, edge1, packs1, sides1,
    rows2, edge2, packs2, sides2, rows3, edge3, packs3, sides3,
    load_sem, list_send, list_recv, a2a_send, a2a_recv, warm_send_sem, warm_recv_sem, skin_send_sem, skin_recv_sem,
    heat_send_sem, heat_recv_sem, send1, recv1, send2, recv2, send3, recv3,
):
    ny = lax.axis_size("gy")
    count = lax.axis_size("gx") * ny
    most = max(2, 2 * NB // count)
    me = lax.axis_index("gx") * ny + lax.axis_index("gy")
    part = NB // PARTS
    pieces = [pl.ds(p * part, part) for p in range(PARTS)]
    moves = [(keeper_far, keeper), (lines_far, lines), (sky_far, sky)]
    moves += [(weights_far.at[piece], weights.at[piece]) for piece in pieces]
    moves += [(sea_far, sea), (h_far, natural.at[0]), (heat_far, heat)]
    moves += [(u_far, natural.at[1]), (v_far, natural.at[2])]
    loads = [
        pltpu.make_async_copy(src, dst, load_sem.at[k]) for k, (src, dst) in enumerate(moves)
    ]
    for load in loads:
        load.start()
    greet_all()
    turning[...] = turning_rows()
    clear_walls((sides1, sides2, sides3))
    blank = jnp.zeros((8, LANES), jnp.float32)
    for f in range(2):
        for tile in range(2):
            state[f, tile, BASE - MARGIN - 8 : BASE - MARGIN] = blank
            state[f, tile, BASE + OX + MARGIN : BASE + OX + MARGIN + 8] = blank
    stage[count * FLUXES * most : count * FLUXES * most + SLOTS] = blank
    loads[0].wait()
    loads[1].wait()
    key_row, key_col, listed = place_blocks(keeper, lines, count)
    for d in range(count):
        listed_out[d] = listed[d : d + 1]
    slots = as_bits(line_numbers((count * SLOTS, NB), 0) == key_row)
    loads[2].wait()
    regrid(sky, weights, partial, loads[3 : 3 + PARTS])
    fill_send(send, warm_send, stage, partial, slots, count, most)
    for load in loads[3 + PARTS : 6 + PARTS]:
        load.wait()
    lat = lax.axis_index("gy") * LANES + lanes(OX)
    inside = (lat > 0) & (lat < ny * LANES - 1)
    shore[8 : 8 + OX] = jnp.where(inside, sea[...].astype(jnp.float32), 0.0)
    fill_edges(heat, natural[0], shore[8 : 8 + OX], heat_edges)
    heats = EdgeSwap(heat_edges, heat_got, heat_send_sem, heat_recv_sem)
    targets = Swap(listed_out, listed_in, list_send, list_recv, 1)
    fluxes = Swap(send, recv, a2a_send, a2a_recv, URGENT * most)
    warmth = Swap(warm_send, warm_recv, warm_send_sem, warm_recv_sem, most)
    skins = Swap(skin_send, skin_recv, skin_send_sem, skin_recv_sem, SLOTS)
    pl.semaphore_wait(pltpu.get_barrier_semaphore(), count - 1)
    heats.start()
    targets.start()
    fluxes.start()
    recv[me] = send[me]
    listed_in[me] = listed_out[me]
    warm_recv[me] = warm_send[me]
    for load in loads[6 + PARTS :]:
        load.wait()
    fill_packs(packs1, [natural[f] for f in range(3)])
    for side in range(2):
        packs1[side, 1] = shore[8 : 8 + OX].astype(jnp.bfloat16)
    for f in range(3):
        fill_rows(rows1, f, natural[f])
    fill_rows(rows1, 3, shore[8 : 8 + OX])
    first = Exchange(rows1, edge1, packs1, sides1, send1, recv1)
    first.start_sides()
    first.start_rows()
    warmth.start()
    place_own(natural, state)
    heats.wait()
    shore[7:8] = heat_got[0, WET_EDGE : WET_EDGE + 1]
    shore[8 + OX : 9 + OX] = heat_got[1, WET_EDGE : WET_EDGE + 1]
    heat_step(heat, heat_got, tall, shore, near, heat_out)
    targets.wait()
    target = read_targets(listed_in, count)
    target_turned = target.T.astype(jnp.bfloat16)
    target = target.astype(jnp.bfloat16)
    fluxes.wait()
    values = read_fluxes(recv, stage, count, most)
    stress = dot(target_turned, jnp.concatenate([values[0], values[1]], axis=1))
    fresh = dot(target_turned, values[2])
    mask = shore[8 : 8 + OX]
    own = [
        WIND_GAIN * stress[:, :LANES] * mask,
        WIND_GAIN * stress[:, LANES:] * mask,
        FRESH_GAIN * fresh * mask,
    ]
    second = Exchange(rows2, edge2, packs2, sides2, send2, recv2)
    fill_packs(packs2, own)
    second.start_sides()
    for f in range(3):
        fill_rows(rows2, f, own[f])
    second.start_rows()
    place_own(own, forces)
    first.wait()
    spread_wet(shore, edge1, sides1, gain)
    spread_fields(edge1, sides1, state, gain)
    height_over_wall(heat_got, state)
    warmth.wait()
    heat_flux = dot(target_turned, received(warm_recv[...], most).astype(jnp.bfloat16))
    surface = heat_out[0] + HEAT_GAIN * heat_flux * shore[8 : 8 + OX]
    heat_out[0] = surface
    band = dot(target, surface.astype(jnp.bfloat16))
    skin_send[...] = band.reshape(count, SLOTS, LANES).astype(jnp.bfloat16)
    skins.start()
    skin_recv[me] = skin_send[me]
    second.wait()
    spread_fields(edge2, sides2, forces, None)
    run_span(state, forces, gain, turning, True)
    third = Exchange(rows3, edge3, packs3, sides3, send3, recv3)
    fill_packs_from_tiles(packs3, state)
    third.start_sides()
    for f in range(3):
        fill_rows_from_tiles(rows3, f, state)
    third.start_rows()
    renew_overlap(state, 0)
    skins.wait()
    slots = as_bits(line_numbers((NB, count * SLOTS), 1) == key_col)
    skin = dot(slots, skin_recv[...].reshape(count * SLOTS, LANES))
    slot8 = lax.broadcasted_iota(jnp.int32, (SLOTS, LANES), 0)
    for g in range(NB // SLOTS):
        rows = slice(g * SLOTS, (g + 1) * SLOTS)
        lines_skin = skin[rows].astype(jnp.bfloat16)
        total = dot(lines_skin, weights[g * SLOTS], 1, 1)
        for n in range(1, SLOTS):
            total = jnp.where(slot8 == n, dot(lines_skin, weights[g * SLOTS + n], 1, 1), total)
        back[rows] = total
    third.wait()
    spread_fields(edge3, sides3, state, None)
    run_span(state, forces, gain, turning, False)
    for f in range(3):
        out[f] = own_part(state, f)


def turning_rows():
    total_y = lax.axis_size("gy") * LANES
    shape = (8, LANES)
    lane = lax.broadcasted_iota(jnp.int32, shape, 1)
    tile = lax.broadcasted_iota(jnp.int32, shape, 0)
    rows = lax.axis_index("gy") * LANES + lane + jnp.where(tile == 0, -MARGIN, MARGIN)
    rows = jnp.where(rows < 0, rows + total_y, jnp.where(rows < total_y, rows, rows - total_y))
    return CORIOLIS * jnp.sin(jnp.pi * ((rows.astype(jnp.float32) + 0.5) / total_y - 0.5))


def hand_over(*refs):
    sources, targets, stores = refs[:3], refs[3:6], refs[6]
    away = [pltpu.make_async_copy(sources[k], targets[k], stores.at[k]) for k in range(3)]
    for copy in away:
        copy.start()
    for copy in away:
        copy.wait()


def per_device(
    sky_interface_transfers,
    coupling_matrix_enlarged,
    piece_keeper_part,
    receiving_part_line,
    marine_point_switch,
    potential_heat_deviation,
    free_marine_lift,
    depth_averaged_uflow,
    depth_averaged_vflow,
):
    count = lax.axis_size("gx") * lax.axis_size("gy")
    most = max(2, 2 * NB // count)
    line = LANES
    half = jnp.bfloat16
    full = jnp.float32

    def boxes(fields, kinds):
        return [
            pltpu.VMEM((2, fields, MARGIN, line), half),
            pltpu.VMEM((2, fields, MARGIN, line), half),
            pltpu.VMEM((2, kinds, OX, line), half),
            pltpu.VMEM((2, kinds, FRAME, line), half),
        ]

    inside = pl.BlockSpec(memory_space=pltpu.VMEM)
    far = pl.BlockSpec(memory_space=pltpu.HBM)
    shapes = (
        jax.ShapeDtypeStruct((NB, OX), full),
        jax.ShapeDtypeStruct((MARINE_STRATA, OX, line), full),
        jax.ShapeDtypeStruct((3, OX, line), full),
    )
    results = pl.pallas_call(
        window_kernel,
        out_shape=shapes,
        in_specs=[far] * 9,
        out_specs=(inside,) * 3,
        scratch_shapes=[
            pltpu.VMEM((FLUXES, NB, OX), half),
            pltpu.VMEM((NB, OX, line), half),
            pltpu.VMEM((1, NB), jnp.int32),
            pltpu.VMEM((1, NB), jnp.int32),
            pltpu.VMEM((OX, line), jnp.int32),
            pltpu.VMEM((MARINE_STRATA, OX, line), full),
            pltpu.VMEM((3, OX, line), full),
            pltpu.VMEM((8, line), full),
            pltpu.VMEM((FLUXES, NB, line), full),
            pltpu.VMEM((count * FLUXES * most + SLOTS, line), full),
            pltpu.VMEM((count, FLUXES * most, line), half),
            pltpu.VMEM((count, FLUXES * most, line), half),
            pltpu.VMEM((count, SLOTS, line), half),
            pltpu.VMEM((count, SLOTS, line), half),
            pltpu.VMEM((count, 1, line), full),
            pltpu.VMEM((count, 1, line), full),
            pltpu.VMEM((count, SLOTS, line), half),
            pltpu.VMEM((count, SLOTS, line), half),
            pltpu.VMEM((4, EDGES, line), full),
            pltpu.VMEM((4, EDGES, line), full),
            pltpu.VMEM((MARINE_STRATA, OX + 16, line), full),
            pltpu.VMEM((2 + MARINE_STRATA, OX, line), full),
            pltpu.VMEM((OX + 16, line), full),
            pltpu.VMEM((3, 2, TALL, line), full),
            pltpu.VMEM((3, 2, TALL, line), full),
            pltpu.VMEM((2, TALL, line), full),
        ]
        + boxes(4, 2)
        + boxes(3, 1)
        + boxes(3, 1)
        + [pltpu.SemaphoreType.DMA((3 + PARTS + 5,))]
        + [pltpu.SemaphoreType.DMA] * 10
        + [pltpu.SemaphoreType.DMA((3,))] * 6,
        compiler_params=pltpu.CompilerParams(
            collective_id=0, has_side_effects=True, vmem_limit_bytes=24 * 1024 * 1024
        ),
        name="window",
    )(
        *[
            pltpu.with_memory_space_constraint(value, pltpu.HBM)
            for value in (
                sky_interface_transfers,
                coupling_matrix_enlarged,
                piece_keeper_part.reshape(1, NB),
                receiving_part_line,
                marine_point_switch,
                potential_heat_deviation,
                free_marine_lift,
                depth_averaged_uflow,
                depth_averaged_vflow,
            )
        ]
    )
    anywhere = pl.BlockSpec(memory_space=pl.ANY)
    return pl.pallas_call(
        hand_over,
        out_shape=shapes,
        in_specs=[anywhere] * 3,
        out_specs=(anywhere,) * 3,
        scratch_shapes=[pltpu.SemaphoreType.DMA((3,))],
        compiler_params=pltpu.CompilerParams(vmem_limit_bytes=8 * 1024 * 1024),
        name="hand_over",
    )(*results)


def solution(mesh):
    in_specs = (
        P(None, "gy", "gx"),
        P("gy", "gx", None),
        P("gx", "gy", None),
        P("gx", "gy"),
        P("gx", "gy"),
        P(None, "gx", "gy"),
        P("gx", "gy"),
        P("gx", "gy"),
        P("gx", "gy"),
    )
    out_specs = (P("gy", "gx"), P(None, "gx", "gy"), P(None, "gx", "gy"))
    return jax.shard_map(
        per_device, mesh=mesh, in_specs=in_specs, out_specs=out_specs, check_vma=False
    )
```
